32 devices in a mesh: gx: 4 (over y, core), gy: 8 (over z, x).
Axes of the slice: x: 2, y: 2, z: 4, core: 2. Of those that a mesh axis runs over, the one named last changes fastest.
Arguments:
- populations: float32 [19, 16, 64, 128], P(None, 'gx', 'gy'), may hold values from 0.004 to 0.8, as said below
- solid: int32 [16, 64, 128], P('gx', 'gy'), may hold values 0 or 1
- base_cell: int32 [3, 4, 8, 2, 768], P(None, 'gx', 'gy'), may hold values from 0 to 127, as said below
- offset: float32 [3, 4, 8, 2, 768], P(None, 'gx', 'gy'), may hold values from 0 to 1
- rest_displacement: float32 [3, 4, 8, 2, 768], P(None, 'gx', 'gy'), may hold values from 0 to 1
- stiffness: float32 [4, 8, 2], P('gx', 'gy'), may hold values from 0.006380062 to 0.063800626
- occupied: int32 [4, 8, 2], P('gx', 'gy'), may hold values from 0 to 1, as said below
- triangles: int32 [1280, 3], replicated, may hold values from 0 to 641, as said below
Outputs:
- populations_out: float32 [19, 16, 64, 128], P(None, 'gx', 'gy')
- offset_out: float32 [3, 4, 8, 2, 768], P(None, 'gx', 'gy')
The draws below stay inside these ranges and needn't reach their ends.
Inputs may be any that keep to these rules, and one draw needn't show every extreme that they name: `populations`: every entry is positive. `base_cell`: component 0 of a vertex stored at index i of gx lies in [i * 4, (i + 1) * 4), component 1 of one stored at index j of gy lies in [j * 8, (j + 1) * 8), component 2 lies below 128. The occupied slots of a device come first; each device has at least one, and some device has all 2. `triangles`: each row holds three different vertex numbers below 642.
All inputs are finite; a program needn't handle non-finite values. No bound on the sum of `solid` on one device may be relied on, other than what follows from the above.
Results may differ from the reference program's by a relative error of at most 0.0001.
Values sent between devices are 32-bit elements; how exact they have to be, the bound alone decides.
A program may use at most 64 MiB of HBM per device.

```python
import math
import jax
import jax.numpy as jnp

CX = 4
CY = 8
CZ = 128
MEMBRANE_SLOTS = 2
VERTS = 642
PADDED_VERTICES = 768
TRIS = 1280
SUBSTEPS = 3
NX = 16
NY = 64
NZ = 128
N_GX = 4
N_GY = 8


DRAW_VELOCITIES = [[0, 0, 0], [1, 0, 0], [-1, 0, 0], [0, 1, 0], [0, -1, 0], [0, 0, 1], [0, 0, -1], [1, 1, 0], [-1, -1, 0], [1, -1, 0], [-1, 1, 0], [1, 0, 1], [-1, 0, -1], [1, 0, -1], [-1, 0, 1], [0, 1, 1], [0, -1, -1], [0, 1, -1], [0, -1, 1]]


DRAW_WEIGHTS = [1.0 / 3.0] + [1.0 / 18.0] * 6 + [1.0 / 36.0] * 12


def draw_populations(key, part):
    key_flow, key_noise = jax.random.split(jax.random.fold_in(key, 11))
    flow = jax.random.uniform(key_flow, (3, NX, NY, NZ), jnp.float32, -0.1, 0.1)
    noise = jax.random.uniform(key_noise, (19, NX, NY, NZ), jnp.float32, 0.7, 1.3)
    halo_layers = []
    for lattice_direction in range(19):
        vector = DRAW_VELOCITIES[lattice_direction]
        along = vector[0] * flow[0] + vector[1] * flow[1] + vector[2] * flow[2]
        halo_layers.append(DRAW_WEIGHTS[lattice_direction] * (1.0 + 3.0 * along) * noise[lattice_direction])
    return jnp.stack(halo_layers)


def draw_base_cell(key, part):
    key_x, key_y, key_z = jax.random.split(jax.random.fold_in(key, 23), 3)
    domain_extent = (N_GX, N_GY, MEMBRANE_SLOTS, PADDED_VERTICES)
    start_x = (jnp.arange(N_GX, dtype=jnp.int32) * CX).reshape(N_GX, 1, 1, 1)
    start_y = (jnp.arange(N_GY, dtype=jnp.int32) * CY).reshape(1, N_GY, 1, 1)
    cell_x = jax.random.randint(key_x, domain_extent, 0, CX, dtype=jnp.int32) + start_x
    cell_y = jax.random.randint(key_y, domain_extent, 0, CY, dtype=jnp.int32) + start_y
    cell_z = jax.random.randint(key_z, domain_extent, 0, CZ, dtype=jnp.int32)
    return jnp.stack([cell_x, cell_y, cell_z])


def draw_occupied(key, part):
    key_level, key_full = jax.random.split(jax.random.fold_in(key, 37))
    level = jax.random.randint(key_level, (N_GX, N_GY), 1, MEMBRANE_SLOTS + 1, dtype=jnp.int32)
    chosen = jax.random.randint(key_full, (), 0, N_GX * N_GY, dtype=jnp.int32)
    device_number = jnp.arange(N_GX * N_GY, dtype=jnp.int32).reshape(N_GX, N_GY)
    level = jnp.where(device_number == chosen, MEMBRANE_SLOTS, level)
    slot_number = jnp.arange(MEMBRANE_SLOTS, dtype=jnp.int32)[None, None, :]
    return (slot_number < level[:, :, None]).astype(jnp.int32)


def draw_triangles(key, part):
    key_first, key_near, distant_key = jax.random.split(jax.random.fold_in(key, 53), 3)
    half = VERTS // 2
    first = jax.random.randint(key_first, (TRIS,), 0, VERTS, dtype=jnp.int32)
    near = jax.random.randint(key_near, (TRIS,), 1, half, dtype=jnp.int32)
    far = jax.random.randint(distant_key, (TRIS,), half, VERTS, dtype=jnp.int32)
    return jnp.stack([first, (first + near) % VERTS, (first + far) % VERTS], axis=1)


def touch_ends(entries, rng, smallest, high):
    place = [jax.random.randint(jax.random.fold_in(rng, axis), (), 0, length) for axis, length in enumerate(entries.shape)]
    main_axis = entries.shape.index(max(entries.shape))
    beside = place[:main_axis] + [(place[main_axis] + 1) % entries.shape[main_axis]] + place[main_axis + 1:]
    return entries.at[tuple(place)].set(smallest).at[tuple(beside)].set(high)


def block_levels(own_key, shape, cuts, low, top_value):
    def one(dim, blocks):
        steps = jax.random.uniform(jax.random.fold_in(jax.random.fold_in(own_key, 6), dim), (blocks,), jnp.float32, low / len(cuts), top_value / len(cuts))
        return jnp.repeat(jnp.exp(steps), shape[dim] // blocks).reshape((-1,) + (1,) * (len(shape) - dim - 1))

    factor_of = one(*cuts[0])
    for cut in cuts[1:]:
        factor_of = factor_of * one(*cut)
    return factor_of


def setup_inputs(seed: int = 0) -> dict:
    key_of = jax.random.split(jax.random.key(seed), 9)
    return {
        "populations": draw_populations(jax.random.fold_in(key_of[8], 71), 0),
        "solid": touch_ends((jax.random.randint(key_of[1], (NX, NY, NZ), 0, 8) < 1).astype(jnp.int32), jax.random.fold_in(key_of[1], 1), 0, 1),
        "base_cell": draw_base_cell(jax.random.fold_in(key_of[8], 71), 0),
        "offset": jnp.clip(1.0 * jax.random.uniform(key_of[3], (3, N_GX, N_GY, MEMBRANE_SLOTS, PADDED_VERTICES), jnp.float32) ** block_levels(key_of[3], (3, N_GX, N_GY, MEMBRANE_SLOTS, PADDED_VERTICES), ((1, 4), (2, 8)), -0.2, 0.2), 0.0, 1.0),
        "rest_displacement": jnp.clip(1.0 * jax.random.uniform(key_of[4], (3, N_GX, N_GY, MEMBRANE_SLOTS, PADDED_VERTICES), jnp.float32) ** block_levels(key_of[4], (3, N_GX, N_GY, MEMBRANE_SLOTS, PADDED_VERTICES), ((1, 4), (2, 8)), -0.2, 0.2), 0.0, 1.0),
        "stiffness": jnp.clip(jnp.exp(math.log(0.063800626) - 2.3025852 * jax.random.uniform(key_of[5], (N_GX, N_GY, MEMBRANE_SLOTS), jnp.float32) ** block_levels(key_of[5], (N_GX, N_GY, MEMBRANE_SLOTS), ((0, 4), (1, 8)), -0.2, 0.2)), 0.006380062, 0.063800626),
        "occupied": draw_occupied(jax.random.fold_in(key_of[8], 71), 0),
        "triangles": draw_triangles(jax.random.fold_in(key_of[8], 71), 0),
    }


VELOCITIES = [[0, 0, 0], [1, 0, 0], [-1, 0, 0], [0, 1, 0], [0, -1, 0], [0, 0, 1], [0, 0, -1], [1, 1, 0], [-1, -1, 0], [1, -1, 0], [-1, 1, 0], [1, 0, 1], [-1, 0, -1], [1, 0, -1], [-1, 0, 1], [0, 1, 1], [0, -1, -1], [0, 1, -1], [0, -1, 1]]
OPPOSITE = [0, 2, 1, 4, 3, 6, 5, 8, 7, 10, 9, 12, 11, 14, 13, 16, 15, 18, 17]
LATTICE_WEIGHTS = [1.0 / 3.0] + [1.0 / 18.0] * 6 + [1.0 / 36.0] * 12
RELAX = 0.8


def kernel_weights(offset):
    return jnp.stack([(1.0 + jnp.cos(math.pi * (stencil_shift - offset) / 2.0)) / 4.0 for stencil_shift in (-1, 0, 1, 2)])


def membrane_force(offset, rest_displacement, stiffness, occupied, triangles):
    strain = offset - rest_displacement
    corners = [triangles[:, 0], triangles[:, 1], triangles[:, 2]]
    summed = strain[..., corners[0]] + strain[..., corners[1]] + strain[..., corners[2]]
    pulled_populations = jnp.zeros_like(strain)
    counts = jnp.zeros((strain.shape[-1],), jnp.float32)
    for corner in corners:
        pulled_populations = pulled_populations.at[..., corner].add(summed)
        counts = counts.at[corner].add(1.0)
    scaling = (stiffness * occupied.astype(jnp.float32))[None, :, :, :, None]
    return scaling * (pulled_populations - 3.0 * counts * strain)


def macro_state(populations, force_cell):
    density = jnp.sum(populations, axis=0)
    velocity_parts = []
    for dimension in range(3):
        moving = force_cell[dimension] * 0.5
        for lattice_direction in range(19):
            component = VELOCITIES[lattice_direction][dimension]
            if component != 0:
                moving = moving + component * populations[lattice_direction]
        velocity_parts.append(moving / density)
    return density, jnp.stack(velocity_parts)


def collide(populations, force_cell, solid):
    density, velocity = macro_state(populations, force_cell)
    squared = velocity[0] * velocity[0] + velocity[1] * velocity[1] + velocity[2] * velocity[2]
    working = velocity[0] * force_cell[0] + velocity[1] * force_cell[1] + velocity[2] * force_cell[2]
    walled = solid != 0
    relaxed = []
    for lattice_direction in range(19):
        vector = VELOCITIES[lattice_direction]
        along = vector[0] * velocity[0] + vector[1] * velocity[1] + vector[2] * velocity[2]
        pushed = vector[0] * force_cell[0] + vector[1] * force_cell[1] + vector[2] * force_cell[2]
        equilibrium = LATTICE_WEIGHTS[lattice_direction] * density * (1.0 + 3.0 * along + 4.5 * along * along - 1.5 * squared)
        source = (1.0 - 0.5 / RELAX) * LATTICE_WEIGHTS[lattice_direction] * (3.0 * (pushed - working) + 9.0 * along * pushed)
        current = populations[lattice_direction]
        updated = current - (current - equilibrium) / RELAX + source
        relaxed.append(jnp.where(walled, populations[OPPOSITE[lattice_direction]], updated))
    return relaxed


def reference(populations, solid, base_cell, offset, rest_displacement, stiffness, occupied, triangles):
    lattice = (NX, NY, NZ)
    cells = NX * NY * NZ
    coordinates = [[(base_cell[dimension] + stencil_shift) % lattice[dimension] for stencil_shift in (-1, 0, 1, 2)] for dimension in range(3)]
    live = occupied.astype(jnp.float32)[None, :, :, :, None]
    for substep in range(SUBSTEPS):
        force_vertex = membrane_force(offset, rest_displacement, stiffness, occupied, triangles)
        kernels = kernel_weights(offset)
        grid = jnp.zeros((3, cells), jnp.float32)
        for first in range(4):
            for second in range(4):
                for third in range(4):
                    index = (coordinates[0][first] * NY + coordinates[1][second]) * NZ + coordinates[2][third]
                    weight = kernels[first][0] * kernels[second][1] * kernels[third][2]
                    grid = grid.at[:, index.reshape(-1)].add((force_vertex * weight[None]).reshape(3, -1))
        force_cell = grid.reshape(3, NX, NY, NZ)
        relaxed = collide(populations, force_cell, solid)
        populations = jnp.stack([jnp.roll(relaxed[lattice_direction], tuple(VELOCITIES[lattice_direction]), axis=(0, 1, 2)) for lattice_direction in range(19)])
        flow = macro_state(populations, force_cell)[1].reshape(3, cells)
        moved = jnp.zeros_like(offset)
        for first in range(4):
            for second in range(4):
                for third in range(4):
                    index = (coordinates[0][first] * NY + coordinates[1][second]) * NZ + coordinates[2][third]
                    weight = kernels[first][0] * kernels[second][1] * kernels[third][2]
                    moved = moved + weight[None] * flow[:, index.reshape(-1)].reshape(offset.shape)
        offset = offset + live * moved
    return populations, offset
```

```python
import functools
import math

import jax
import jax.numpy as jnp
from jax import lax
from jax.experimental import pallas as pl
from jax.experimental.pallas import tpu as pltpu
from jax.sharding import PartitionSpec as P

SUBSTEPS = 3
VELOCITIES = [
    (0, 0, 0), (1, 0, 0), (-1, 0, 0), (0, 1, 0), (0, -1, 0), (0, 0, 1), (0, 0, -1),
    (1, 1, 0), (-1, -1, 0), (1, -1, 0), (-1, 1, 0), (1, 0, 1), (-1, 0, -1), (1, 0, -1),
    (-1, 0, 1), (0, 1, 1), (0, -1, -1), (0, 1, -1), (0, -1, 1),
]
OPPOSITE = [0, 2, 1, 4, 3, 6, 5, 8, 7, 10, 9, 12, 11, 14, 13, 16, 15, 18, 17]
LATTICE_WEIGHTS = [1.0 / 3.0] + [1.0 / 18.0] * 6 + [1.0 / 36.0] * 12
RELAX = 0.8
XS = {s: [q for q in range(19) if VELOCITIES[q][0] == s] for s in (1, -1)}
YS = {s: [q for q in range(19) if VELOCITIES[q][1] == s] for s in (1, -1)}
CORNER = {(v[0], v[1]): q for q, v in enumerate(VELOCITIES) if v[0] and v[1]}
DIRS = [(1, 0), (-1, 0), (0, 1), (0, -1), (1, 1), (1, -1), (-1, 1), (-1, -1)]
MESH = pl.DeviceIdType.MESH
NT = (((1,), (1,)), ((), ()))
NN = (((1,), (0,)), ((), ()))


def mm(a, b, dims):
    return lax.dot_general(a, b, dims, preferred_element_type=jnp.float32)


def split(value):
    high = value.astype(jnp.bfloat16)
    low = (value - high.astype(jnp.float32)).astype(jnp.bfloat16)
    return high, low


def quarter_sine(t):
    t = t - 4.0 * jnp.floor(t * 0.25 + 0.5)
    t = jnp.where(t > 1.0, 2.0 - t, jnp.where(t < -1.0, -2.0 - t, t))
    x = t * (math.pi / 2.0)
    u = x * x
    p = 1.0 / 6227020800.0
    for c in (-1.0 / 39916800.0, 1.0 / 362880.0, -1.0 / 5040.0, 1.0 / 120.0, -1.0 / 6.0, 1.0):
        p = p * u + c
    return x * p


def table(rows, base, kernels):
    cells = lax.broadcasted_iota(jnp.int32, (rows, base.shape[1]), 0)
    d = (cells - base + 1) & (rows - 1)
    out = jnp.where(d == 3, kernels[3], 0.0)
    for s in (2, 1, 0):
        out = jnp.where(d == s, kernels[s], out)
    return out


def moments(pops):
    density = functools.reduce(lambda a, b: a + b, pops)
    momentum = []
    for a in range(3):
        plus = [pops[q] for q in range(19) if VELOCITIES[q][a] == 1]
        minus = [pops[q] for q in range(19) if VELOCITIES[q][a] == -1]
        momentum.append(
            functools.reduce(lambda a, b: a + b, plus)
            - functools.reduce(lambda a, b: a + b, minus)
        )
    return density, momentum


def collide(pops, force, walled):
    density, momentum = moments(pops)
    inverse = 1.0 / density
    u = [(momentum[a] + 0.5 * force[a]) * inverse for a in range(3)]
    squared = u[0] * u[0] + u[1] * u[1] + u[2] * u[2]
    working = u[0] * force[0] + u[1] * force[1] + u[2] * force[2]
    base = 1.0 - 1.5 * squared
    relaxed = []
    for q in range(19):
        vector = VELOCITIES[q]
        along, pushed = jnp.zeros_like(density), jnp.zeros_like(density)
        for a in range(3):
            if vector[a] == 1:
                along, pushed = along + u[a], pushed + force[a]
            elif vector[a] == -1:
                along, pushed = along - u[a], pushed - force[a]
        w = LATTICE_WEIGHTS[q]
        equilibrium = (w * density) * (base + along * (3.0 + 4.5 * along))
        source = ((1.0 - 0.5 / RELAX) * w) * (3.0 * (pushed - working) + 9.0 * along * pushed)
        updated = pops[q] - (pops[q] - equilibrium) * (1.0 / RELAX) + source
        relaxed.append(jnp.where(walled, pops[OPPOSITE[q]], updated))
    return relaxed


def roll(x, shift, axis):
    size = x.shape[axis]
    shift = shift % size
    return x if shift == 0 else pltpu.roll(x, shift, axis)


def row_mask(start, rows, depth):
    sub = lax.broadcasted_iota(jnp.int32, (8, depth), 0)
    return ((sub - start) & 7) < rows


def pack(tiles, start, rows):
    per, out = 8 // rows, []
    for g in range(0, len(tiles), per):
        acc = tiles[g]
        for k, tile in enumerate(tiles[g + 1 : g + per], 1):
            mask = row_mask(start + k * rows, rows, tile.shape[1])
            acc = jnp.where(mask, roll(tile, k * rows, 0), acc)
        out.append(acc)
    return out


def unpack(load, count, rows):
    per = 8 // rows
    return [roll(load(k // per), -(k % per) * rows, 0) for k in range(count)]


def packed(count, rows):
    return -(-count // (8 // rows))


def force_planes(sx, rows_x):
    return {1: [rows_x, rows_x + 1], -1: [-1], 0: list(range(rows_x))}[sx]


def moment_planes(sx, rows_x):
    return {1: [rows_x - 1, rows_x], -1: [-1, 0, 1], 0: list(range(-1, rows_x + 1))}[sx]


def landing(x, sx, rows_x):
    return x - sx * rows_x


def force_size(sx, sy, rows_x):
    n = 3 * len(force_planes(sx, rows_x))
    return {0: n, 1: packed(n, 2), -1: packed(n, 1)}[sy]


def moment_size(sx, sy, rows_x):
    n = 4 * len(moment_planes(sx, rows_x))
    return {0: n + packed(n, 2), 1: packed(n, 2), -1: packed(n, 1) + packed(n, 2)}[sy]


def total_of(parts):
    return functools.reduce(lambda a, b: a + b, parts)


def body_kernel(
    peers_x, peers_y,
    pops_hbm, solid_hbm, base_hbm, offset_hbm, rest_hbm, stiff_hbm, occ_hbm, tri_hbm,
    pops_out, offset_out,
    solid_ref, base_ref, offset_ref, rest_ref, stiff_ref, occ_ref, tri_ref,
    incidence, lap, off, spread, moved_ref, wide,
    *scratch,
):
    recv_force, recv_pops, recv_mom = scratch[0:8], scratch[8:16], scratch[16:24]
    send_force, send_pops, send_mom = scratch[24:32], scratch[32:40], scratch[40:48]
    send_px, send_py, send_pc = send_pops[0:2], send_pops[2:4], send_pops[4:8]
    send_sem, recv_sem, load_sem = scratch[48:51]
    rows_x = pops_out.shape[1]
    depth = pops_out.shape[3]
    slots, padded = base_ref.shape[1], base_ref.shape[2]
    vertices = slots * padded
    planes = rows_x + 3
    ix, iy = lax.axis_index("gx"), lax.axis_index("gy")
    peer = [((ix + sx + peers_x) % peers_x, (iy + sy + peers_y) % peers_y) for sx, sy in DIRS]

    loads = [
        pltpu.make_async_copy(src, dst, load_sem.at[k])
        for k, (src, dst) in enumerate((
            (tri_hbm, tri_ref), (offset_hbm, offset_ref), (rest_hbm, rest_ref),
            (base_hbm, base_ref), (stiff_hbm, stiff_ref), (occ_hbm, occ_ref),
            (solid_hbm, solid_ref), (pops_hbm, pops_out),
        ))
    ]
    for x in loads:
        x.start()
    barrier = pltpu.get_barrier_semaphore()
    for p in peer:
        pl.semaphore_signal(barrier, inc=1, device_id=p, device_id_type=MESH)

    loads[0].wait()
    faces = tri_ref.shape[1]
    for start in range(0, faces, 256):
        stop = min(start + 256, faces)
        ids = lax.broadcasted_iota(jnp.int32, (padded, stop - start), 0)
        corner = [tri_ref[k : k + 1, start:stop] for k in range(3)]
        hit = (ids == corner[0]) | (ids == corner[1]) | (ids == corner[2])
        incidence[:, start:stop] = jnp.where(hit, 1.0, 0.0).astype(jnp.bfloat16)
    for x in loads[1:6]:
        x.wait()

    def build_laplacian():
        pairs = None
        for start in range(0, faces, 256):
            part = incidence[:, start : min(start + 256, faces)]
            part = mm(part, part, NT)
            pairs = part if pairs is None else pairs + part
        same = lax.broadcasted_iota(jnp.int32, pairs.shape, 0) == lax.broadcasted_iota(
            jnp.int32, pairs.shape, 1
        )
        lap_high, lap_low = split(jnp.where(same, -2.0 * pairs, pairs))
        lap[0] = lap_high
        lap[1] = lap_low

    def flat(ref):
        return jnp.concatenate([ref[:, m, :] for m in range(slots)], axis=1)

    base = flat(base_ref)
    base_x = base[0:1] - ix * rows_x
    base_y = base[1:2] - iy * pops_out.shape[2]
    base_z = base[2:3]
    live = jnp.concatenate(
        [jnp.full((1, padded), occ_ref[m].astype(jnp.float32)) for m in range(slots)], axis=1
    )
    scale = live * jnp.concatenate(
        [jnp.full((1, padded), stiff_ref[m]) for m in range(slots)], axis=1
    )
    off[...] = flat(offset_ref)
    sub = lax.broadcasted_iota(jnp.int32, (8, depth), 0)

    def copy(step, stage, d, src, dst):
        return pltpu.make_async_remote_copy(
            src_ref=src, dst_ref=dst.at[step], send_sem=send_sem.at[step, stage, d],
            recv_sem=recv_sem.at[step, stage, d], device_id=peer[d], device_id_type=MESH,
        )

    groups = ((send_force, recv_force), (send_mom, recv_mom), (send_pops, recv_pops))

    def copies(step, stage):
        src, dst = groups[stage]
        return [copy(step, stage, d, src[d].at[step], dst[d]) for d in range(8)]

    def launch(step, stage):
        sends = copies(step, stage)

        @pl.when(iy % 2 == 1)
        def _():
            for d in (4, 6, 2, 5, 7, 3, 0, 1):
                sends[d].start()

        @pl.when(iy % 2 == 0)
        def _():
            for d in (5, 7, 3, 4, 6, 2, 0, 1):
                sends[d].start()

    def arrive(step, stage):
        for x in copies(step, stage):
            x.wait_recv()

    def finish_pops(step):
        arrive(step, 2)
        from_y = {1: recv_pops[2][step], -1: recv_pops[3][step]}
        for q in range(19):
            sx, sy, _ = VELOCITIES[q]
            value = moved_ref[q]
            edge_row = sub == (0 if sy == 1 else 7)
            if sy:
                value = jnp.where(edge_row, roll(from_y[sy], -YS[sy].index(q), 1), value)
            if sx:
                side = recv_pops[0 if sx == 1 else 1][step, XS[sx].index(q)]
                if sy:
                    side = jnp.where(edge_row, recv_pops[DIRS.index((sx, sy))][step], side)
                if sx == 1:
                    value = jnp.concatenate([side[None], value[:-1]], axis=0)
                else:
                    value = jnp.concatenate([value[1:], side[None]], axis=0)
            pops_out[q] = value

    def stacked(value):
        high = value.astype(jnp.bfloat16).astype(jnp.float32)
        return jnp.concatenate([high, value - high], axis=0).astype(jnp.bfloat16)

    def substep(step, carry, first=False):
        now = off[...]
        strain = now - flat(rest_ref)
        six = jnp.concatenate(
            [strain[:, m * padded : (m + 1) * padded] for m in range(slots)], axis=0
        )
        if first:
            summed = mm(stacked(six), incidence[...], NN)
            summed = summed[0 : 3 * slots] + summed[3 * slots :]
            both = jnp.concatenate(
                [stacked(summed), jnp.ones((1, faces), jnp.bfloat16)], axis=0
            )
            pulled = mm(both, incidence[...], NT)
            count = pulled[6 * slots :]
            pulled = pulled[0 : 3 * slots] + pulled[3 * slots : 6 * slots]
            pulled = pulled - 3.0 * count * six
        else:
            both = stacked(six)
            pulled = mm(both, lap[0], NN) + mm(both, lap[1], NN)
            pulled = pulled[0 : 3 * slots] + pulled[3 * slots :]
        force_v = scale * jnp.concatenate(
            [pulled[3 * m : 3 * m + 3] for m in range(slots)], axis=1
        )
        s = quarter_sine(now) * 0.25
        c = quarter_sine(now + 1.0) * 0.25
        kernels = (0.25 - s, 0.25 + c, 0.25 + s, 0.25 - c)
        table_x = table(8, base_x, [k[0:1] for k in kernels])
        table_y = table(16, base_y, [k[1:2] for k in kernels])
        deep_high, deep_low = split(table(depth, base_z, [k[2:3] for k in kernels]))
        deep = jnp.concatenate([deep_high, deep_low], axis=0)
        tiles_of = {}

        def spread_tiles(names, start):
            for n in range(0, len(names), 2):
                blocks = [
                    (force_v[a : a + 1] * table_x[x & 7 : (x & 7) + 1])
                    * table_y[8 * t : 8 * t + 8]
                    for x, a, t in names[n : n + 2]
                ]
                high, low = split(jnp.concatenate(blocks, axis=0))
                row = start + 8 * n
                spread[0, row : row + 16, :] = high
                spread[1, row : row + 16, :] = low
            stop = start + 8 * len(names)
            first = mm(spread[0, start:stop], deep, NT)
            total = first[:, :depth] + first[:, depth:]
            total = total + mm(spread[1, start:stop], deep_high, NT)
            for n, name in enumerate(names):
                tiles_of[name] = total[8 * n : 8 * n + 8]

        outer = [(x, a, t) for x in (rows_x, rows_x + 1, -1) for a in range(3) for t in (0, 1)]
        outer += [(x, a, 1) for x in range(rows_x) for a in range(3)]
        spread_tiles(outer, 0)
        for d, (sx, sy) in enumerate(DIRS):
            tiles = [
                tiles_of[x, a, 0 if sy == 0 else 1]
                for x in force_planes(sx, rows_x) for a in range(3)
            ]
            if sy:
                tiles = pack(tiles, 0 if sy == 1 else 7, 2 if sy == 1 else 1)
            for k, tile in enumerate(tiles):
                send_force[d][step, k] = tile
        if first:
            pl.semaphore_wait(barrier, len(peer))
        launch(step, 0)
        spread_tiles([(x, a, 0) for x in range(rows_x) for a in range(3)], 8 * len(outer))

        if first:
            build_laplacian()
            loads[6].wait()
            loads[7].wait()
        else:
            finish_pops(step - 1)

        arrive(step, 0)
        parts = {(x, a): [tiles_of[x, a, 0]] for x in range(rows_x) for a in range(3)}
        for d, (sx, sy) in enumerate(DIRS):
            names = [
                (landing(x, sx, rows_x), a) for x in force_planes(sx, rows_x) for a in range(3)
            ]
            load = lambda k, d=d: recv_force[d][step, k]
            if sy == 0:
                tiles = [load(k) for k in range(len(names))]
            else:
                start, rows = (0, 2) if sy == 1 else (7, 1)
                mask = row_mask(start, rows, depth)
                tiles = [jnp.where(mask, t, 0.0) for t in unpack(load, len(names), rows)]
            for name, tile in zip(names, tiles):
                parts[name].append(tile)
        force = [
            jnp.stack([total_of(parts[x, a]) for x in range(rows_x)]) for a in range(3)
        ]

        relaxed = collide([pops_out[q] for q in range(19)], force, solid_ref[...] != 0)
        moved = [
            roll(roll(relaxed[q], VELOCITIES[q][2], 2), VELOCITIES[q][1], 1) for q in range(19)
        ]
        for q in range(19):
            moved_ref[q] = moved[q]
        nothing = jnp.zeros((1, 8, depth), jnp.float32)
        rho, mz = {}, {}
        for cx in (-1, 0, 1):
            for cy in (-1, 0, 1):
                members = [q for q in range(19) if VELOCITIES[q][:2] == (cx, cy)]
                pad = lambda v: jnp.concatenate(
                    [nothing] * (1 + cx) + [v] + [nothing] * (1 - cx), axis=0
                )
                rho[cx, cy] = pad(total_of([moved[q] for q in members]))
                up = [moved[q] for q in members if VELOCITIES[q][2] == 1]
                down = [moved[q] for q in members if VELOCITIES[q][2] == -1]
                if up:
                    mz[cx, cy] = pad(total_of(up) - total_of(down))
        first_row, last_row = sub == 0, sub == 7
        own = {}
        zero = jnp.zeros((rows_x + 2, 8, depth), jnp.float32)
        fields = []
        for cy in (0, 1, -1):
            dens = rho[-1, cy] + rho[0, cy] + rho[1, cy]
            deep_m = [mz[cx, cy] for cx in (-1, 0, 1) if (cx, cy) in mz]
            fields.append((
                dens, rho[1, cy] - rho[-1, cy], zero if cy == 0 else cy * dens, total_of(deep_m)
            ))
        for c in range(4):
            mid, up, down = (fields[g][c] for g in range(3))
            near = mid + jnp.where(first_row, 0.0, up) + jnp.where(last_row, 0.0, down)
            if c:
                half = 0.5 * force[c - 1]
                near = near + jnp.concatenate([nothing, half, nothing], axis=0)
            far = jnp.where(first_row, up, jnp.where(last_row, down, 0.0))
            for x in range(-1, rows_x + 1):
                own[x, c] = (near[x + 1], far[x + 1])
        for d, (sx, sy) in enumerate(DIRS):
            names = [(x, c) for x in moment_planes(sx, rows_x) for c in range(4)]
            near, far = [own[n][0] for n in names], [own[n][1] for n in names]
            if sy == 0:
                tiles = near + pack(far, 7, 2)
            elif sy == 1:
                tiles = pack([jnp.where(last_row, a, b) for a, b in zip(near, far)], 7, 2)
            else:
                tiles = pack(far, 7, 1) + pack(near, 0, 2)
            for k, tile in enumerate(tiles):
                send_mom[d][step, k] = tile
        launch(step, 1)
        for n, sx in enumerate((1, -1)):
            edge = rows_x - 1 if sx == 1 else 0
            for k, q in enumerate(XS[sx]):
                send_px[n][step, k] = moved[q][edge]
        for n, sy in enumerate((1, -1)):
            rows_kept = moved[YS[sy][0]]
            start = 0 if sy == 1 else 7
            for k, q in enumerate(YS[sy][1:], 1):
                rows_kept = jnp.where(sub == (start + k) % 8, roll(moved[q], k, 1), rows_kept)
            send_py[n][step] = rows_kept
        for n, (sx, sy) in enumerate(DIRS[4:]):
            send_pc[n][step] = moved[CORNER[sx, sy]][rows_x - 1 if sx == 1 else 0]
        launch(step, 2)
        arrive(step, 1)
        reach = [x for x in range(rows_x + 2)] + [-1]
        near = {(x, c): [] for x in reach for c in range(4)}
        far = {(x, c): [] for x in reach for c in range(4)}
        for name, (a, b) in own.items():
            near[name].append(a)
            far[name].append(b)
        two, edges, one = row_mask(0, 2, depth), row_mask(7, 2, depth), row_mask(7, 1, depth)
        for d, (sx, sy) in enumerate(DIRS):
            names = [
                (landing(x, sx, rows_x), c)
                for x in moment_planes(sx, rows_x) for c in range(4)
            ]
            count = len(names)
            load = lambda k, d=d: recv_mom[d][step, k]
            if sy == 0:
                a = [load(k) for k in range(count)]
                b = unpack(lambda k: load(count + k), count, 2)
                b = [jnp.where(edges, t, 0.0) for t in b]
            elif sy == 1:
                both_rows = unpack(load, count, 2)
                a = [jnp.where(first_row, t, 0.0) for t in both_rows]
                b = [jnp.where(last_row, t, 0.0) for t in both_rows]
            else:
                skip = packed(count, 1)
                a = [jnp.where(one, t, 0.0) for t in unpack(load, count, 1)]
                b = unpack(lambda k: load(skip + k), count, 2)
                b = [jnp.where(two, t, 0.0) for t in b]
            for name, p, r in zip(names, a, b):
                near[name].append(p)
                far[name].append(r)
        used = row_mask(7, 3, depth)
        for i, x in enumerate(reach):
            for t, side in enumerate((near, far)):
                dens = total_of(side[x, 0])
                if t:
                    dens = jnp.where(used, dens, 1.0)
                inverse = 1.0 / dens
                for a in range(3):
                    wide[i, a, t] = total_of(side[x, a + 1]) * inverse
        wide_high, wide_low = split(wide[...].reshape(planes * 3 * 16, depth))
        twice = jnp.concatenate([wide_high, wide_high], axis=1)
        along = mm(twice, deep, NN) + mm(wide_low, deep_high, NN)
        along = along.reshape(planes, 3, 16, vertices)
        drift, order = [], list(range(rows_x + 2)) + [7]
        for a in range(3):
            acc = along[0, a] * table_x[0:1]
            for i, x in enumerate(order[1:], 1):
                acc = acc + along[i, a] * table_x[x : x + 1]
            drift.append(jnp.sum(acc * table_y, axis=0, keepdims=True))
        off[...] = now + live * jnp.concatenate(drift, axis=0)
        return carry

    substep(0, 0, True)
    lax.fori_loop(1, SUBSTEPS, substep, 0)
    finish_pops(SUBSTEPS - 1)

    for m in range(slots):
        offset_out[:, m, :] = off[:, m * padded : (m + 1) * padded]

    def drain(step, carry):
        for stage in range(3):
            for x in copies(step, stage):
                x.wait_send()
        return carry

    lax.fori_loop(0, SUBSTEPS, drain, 0)


def write_kernel(pops_ref, offset_ref, pops_out, offset_out, sem):
    copies = [
        pltpu.make_async_copy(pops_ref, pops_out, sem.at[0]),
        pltpu.make_async_copy(offset_ref, offset_out, sem.at[1]),
    ]
    for x in copies:
        x.start()
    for x in copies:
        x.wait()


def local(mesh, populations, solid, base_cell, offset, rest, stiffness, occupied, triangles):
    rows_x, rows_y, depth = populations.shape[1:]
    slots, padded = offset.shape[3:]
    assert rows_y == 8 and rows_x == 4 and depth & (depth - 1) == 0
    vertices, planes = slots * padded, rows_x + 3
    S = SUBSTEPS
    f32, bf16 = jnp.float32, jnp.bfloat16
    tile = (8, depth)
    pop_shapes = [(5,)] * 2 + [(rows_x,)] * 2 + [()] * 4
    V = lambda shape, dtype=f32: pltpu.VMEM(shape, dtype)
    small = (3, slots, padded)
    i32 = jnp.int32
    scratch = [
        V(solid.shape, i32), V(small, i32), V(small), V(small),
        pltpu.SMEM((slots,), f32), pltpu.SMEM((slots,), i32), V(triangles.shape[::-1], i32),
        V((padded, triangles.shape[0]), bf16),
        V((2, padded, padded), bf16), V((3, vertices)),
        V((2, planes * 48, vertices), bf16),
        V((19, rows_x) + tile), V((planes, 3, 2) + tile),
    ]
    for _ in ("receive", "send"):
        scratch += [V((S, force_size(*d, rows_x)) + tile) for d in DIRS]
        scratch += [V((S,) + p + tile) for p in pop_shapes]
        scratch += [V((S, moment_size(*d, rows_x)) + tile) for d in DIRS]
    scratch += [pltpu.SemaphoreType.DMA((S, 3, 8)), pltpu.SemaphoreType.DMA((S, 3, 8))]
    scratch += [pltpu.SemaphoreType.DMA((8,))]
    vmem = pl.BlockSpec(memory_space=pltpu.VMEM)
    hbm = pl.BlockSpec(memory_space=pltpu.HBM)
    pops, moved = pl.pallas_call(
        functools.partial(body_kernel, mesh.shape["gx"], mesh.shape["gy"]),
        out_shape=(pltpu.VMEM(populations.shape, f32), pltpu.VMEM(small, f32)),
        in_specs=[hbm] * 8,
        out_specs=(vmem, vmem),
        scratch_shapes=scratch,
        compiler_params=pltpu.CompilerParams(
            collective_id=0, has_side_effects=True, vmem_limit_bytes=24 * 1024 * 1024
        ),
    )(*[
        pltpu.with_memory_space_constraint(x, pltpu.HBM)
        for x in (
            populations, solid, base_cell.reshape(small), offset.reshape(small),
            rest.reshape(small), stiffness.reshape(slots), occupied.reshape(slots), triangles.T,
        )
    ])
    pops, moved = pl.pallas_call(
        write_kernel,
        out_shape=(
            jax.ShapeDtypeStruct(populations.shape, f32), jax.ShapeDtypeStruct(small, f32),
        ),
        in_specs=[pl.BlockSpec(memory_space=pl.ANY)] * 2,
        out_specs=(hbm, hbm),
        scratch_shapes=[pltpu.SemaphoreType.DMA((2,))],
        compiler_params=pltpu.CompilerParams(vmem_limit_bytes=1024 * 1024),
    )(pops, moved)
    return pops, moved.reshape(offset.shape)


def solution(mesh):
    in_specs = (
        P(None, "gx", "gy", None),
        P("gx", "gy", None),
        P(None, "gx", "gy", None, None),
        P(None, "gx", "gy", None, None),
        P(None, "gx", "gy", None, None),
        P("gx", "gy", None),
        P("gx", "gy", None),
        P(),
    )
    out_specs = (P(None, "gx", "gy", None), P(None, "gx", "gy", None, None))
    return jax.shard_map(
        functools.partial(local, mesh), mesh=mesh, in_specs=in_specs, out_specs=out_specs,
        check_vma=False,
    )
```

```python
import functools
import math

import jax
import jax.numpy as jnp
from jax import lax
from jax.experimental import pallas as pl
from jax.experimental.pallas import tpu as pltpu
from jax.sharding import PartitionSpec as P

SUBSTEPS = 3
VELOCITIES = [
    (0, 0, 0), (1, 0, 0), (-1, 0, 0), (0, 1, 0), (0, -1, 0), (0, 0, 1), (0, 0, -1),
    (1, 1, 0), (-1, -1, 0), (1, -1, 0), (-1, 1, 0), (1, 0, 1), (-1, 0, -1), (1, 0, -1),
    (-1, 0, 1), (0, 1, 1), (0, -1, -1), (0, 1, -1), (0, -1, 1),
]
OPPOSITE = [0, 2, 1, 4, 3, 6, 5, 8, 7, 10, 9, 12, 11, 14, 13, 16, 15, 18, 17]
LATTICE_WEIGHTS = [1.0 / 3.0] + [1.0 / 18.0] * 6 + [1.0 / 36.0] * 12
RELAX = 0.8
CHUNK = 256
XS = {s: [q for q in range(19) if VELOCITIES[q][0] == s] for s in (1, -1)}
YS = {s: [q for q in range(19) if VELOCITIES[q][1] == s] for s in (1, -1)}
CORNER = {(v[0], v[1]): q for q, v in enumerate(VELOCITIES) if v[0] and v[1]}
DIRS = [(1, 0), (-1, 0), (0, 1), (0, -1), (1, 1), (1, -1), (-1, 1), (-1, -1)]
MESH = pl.DeviceIdType.MESH
NT = (((1,), (1,)), ((), ()))
NN = (((1,), (0,)), ((), ()))


def mm(a, b, dims):
    return lax.dot_general(a, b, dims, preferred_element_type=jnp.float32)


def split(value):
    high = value.astype(jnp.bfloat16)
    low = (value - high.astype(jnp.float32)).astype(jnp.bfloat16)
    return high, low


def quarter_sine(t):
    t = t - 4.0 * jnp.floor(t * 0.25 + 0.5)
    t = jnp.maximum(jnp.minimum(t, 2.0 - t), -2.0 - t)
    x = t * (math.pi / 2.0)
    u = x * x
    p = 1.0 / 6227020800.0
    for c in (-1.0 / 39916800.0, 1.0 / 362880.0, -1.0 / 5040.0, 1.0 / 120.0, -1.0 / 6.0, 1.0):
        p = p * u + c
    return x * p


def distance(rows, base):
    cells = lax.broadcasted_iota(jnp.int32, (rows, base.shape[1]), 0)
    return (cells - base + 1) & (rows - 1)


def moments(pops):
    density = functools.reduce(lambda a, b: a + b, pops)
    momentum = []
    for a in range(3):
        plus = [pops[q] for q in range(19) if VELOCITIES[q][a] == 1]
        minus = [pops[q] for q in range(19) if VELOCITIES[q][a] == -1]
        momentum.append(
            functools.reduce(lambda a, b: a + b, plus)
            - functools.reduce(lambda a, b: a + b, minus)
        )
    return density, momentum


def settle(pops, walled):
    density, momentum = moments(pops)
    kept = 1.0 - 1.0 / RELAX
    still = [jnp.where(walled, pops[OPPOSITE[q]], kept * pops[q]) for q in range(19)]
    return density, momentum, still


def collide(density, momentum, still, force, walled):
    inverse = 1.0 / density
    rate, keep = 1.0 / RELAX, 1.0 - 0.5 / RELAX
    n = [momentum[a] + 0.5 * force[a] for a in range(3)]
    u = [jnp.where(walled, 0.0, n[a] * inverse) for a in range(3)]
    squared = u[0] * n[0] + u[1] * n[1] + u[2] * n[2]
    working = u[0] * force[0] + u[1] * force[1] + u[2] * force[2]
    even = rate * density - (1.5 * rate) * squared - (3.0 * keep) * working
    w = LATTICE_WEIGHTS[1]
    odd = [(3.0 * rate * w) * n[a] + (3.0 * keep * w) * force[a] for a in range(3)]
    twice = [(4.5 * rate * w) * n[a] + (9.0 * keep * w) * force[a] for a in range(3)]
    even = jnp.where(walled, 0.0, even)
    odd = [jnp.where(walled, 0.0, x) for x in odd]
    axis_even, half_even = w * even, (0.5 * w) * even
    half_odd, half_twice = [0.5 * x for x in odd], [0.5 * x for x in twice]

    def dot(vector, values):
        terms = [(vector[a], values[a]) for a in range(3) if vector[a]]
        out = terms[0][1] if terms[0][0] == 1 else -terms[0][1]
        for sign, value in terms[1:]:
            out = out + value if sign == 1 else out - value
        return out

    fresh = {0: LATTICE_WEIGHTS[0] * even}
    for q in range(1, 19, 2):
        vector = VELOCITIES[q]
        diagonal = sum(abs(v) for v in vector) == 2
        push = dot(vector, half_odd if diagonal else odd)
        mid = (half_even if diagonal else axis_even) + dot(vector, u) * dot(
            vector, half_twice if diagonal else twice
        )
        fresh[q], fresh[OPPOSITE[q]] = mid + push, mid - push
    return [still[q] + fresh[q] for q in range(19)]


def roll(x, shift, axis):
    size = x.shape[axis]
    shift = shift % size
    return x if shift == 0 else pltpu.roll(x, shift, axis)


def row_mask(start, rows, depth):
    sub = lax.broadcasted_iota(jnp.int32, (8, depth), 0)
    return ((sub - start) & 7) < rows


def pack(tiles, start, rows):
    per, out = 8 // rows, []
    for g in range(0, len(tiles), per):
        acc = tiles[g]
        for k, tile in enumerate(tiles[g + 1 : g + per], 1):
            mask = row_mask(start + k * rows, rows, tile.shape[1])
            acc = jnp.where(mask, roll(tile, k * rows, 0), acc)
        out.append(acc)
    return out


def unpack(load, count, rows):
    per = 8 // rows
    return [roll(load(k // per), -(k % per) * rows, 0) for k in range(count)]


def packed(count, rows):
    return -(-count // (8 // rows))


def force_planes(sx, rows_x):
    return {1: [rows_x, rows_x + 1], -1: [-1], 0: list(range(rows_x))}[sx]


def moment_planes(sx, rows_x):
    return {1: [rows_x - 1, rows_x], -1: [-1, 0, 1], 0: list(range(-1, rows_x + 1))}[sx]


def landing(x, sx, rows_x):
    return x - sx * rows_x


def force_size(sx, sy, rows_x):
    n = 3 * len(force_planes(sx, rows_x))
    return n if sy == 0 else -(-n * (2 if sy == 1 else 1) // 8)


def moment_size(sx, sy, rows_x):
    n = 4 * len(moment_planes(sx, rows_x))
    return {0: n + packed(n, 2), 1: packed(n, 2), -1: packed(n, 1) + packed(n, 2)}[sy]


def stage_sizes(rows_x, stage):
    force = [force_size(*d, rows_x) for d in DIRS]
    moment = [moment_size(*d, rows_x) for d in DIRS]
    pops = [len(XS[1])] * 2 + [rows_x] * 2 + [1] * 4
    sizes = (force, moment, pops)
    return sum(sum(x) for x in sizes[:stage]), sizes[stage]


def total_of(parts):
    return functools.reduce(lambda a, b: a + b, parts)


def body_kernel(
    peers_x, peers_y,
    pops_hbm, solid_hbm, base_hbm, offset_hbm, rest_hbm, stiff_hbm, occ_hbm, tri_hbm,
    pops_out, offset_out,
    solid_ref, base_ref, offset_ref, rest_ref, stiff_ref, occ_ref, tri_ref,
    incidence, lap, off, spread, deep, masks, masks_z, moved_ref, wide,
    send_buf, recv_buf, send_sem, recv_sem, load_sem,
):
    rows_x = pops_out.shape[1]
    depth = pops_out.shape[3]
    slots, padded = base_ref.shape[1], base_ref.shape[2]
    vertices = slots * padded
    chunks = [slice(k, min(k + CHUNK, vertices)) for k in range(0, vertices, CHUNK)]
    ix, iy = lax.axis_index("gx"), lax.axis_index("gy")
    peer = [((ix + sx + peers_x) % peers_x, (iy + sy + peers_y) % peers_y) for sx, sy in DIRS]

    loads = [
        pltpu.make_async_copy(src, dst, load_sem.at[k])
        for k, (src, dst) in enumerate((
            (tri_hbm, tri_ref), (offset_hbm, offset_ref), (rest_hbm, rest_ref),
            (base_hbm, base_ref), (stiff_hbm, stiff_ref), (occ_hbm, occ_ref),
            (solid_hbm, solid_ref), (pops_hbm, pops_out),
        ))
    ]
    for x in loads:
        x.start()
    barrier = pltpu.get_barrier_semaphore()
    for p in peer:
        pl.semaphore_signal(barrier, inc=1, device_id=p, device_id_type=MESH)

    for x in loads[:6]:
        x.wait()
    faces = tri_ref.shape[1]
    parts = [slice(k, min(k + 256, faces)) for k in range(0, faces, 256)]

    def build_laplacian():
        pairs = None
        for cut in parts:
            part = mm(incidence[:, cut], incidence[:, cut], NT)
            pairs = part if pairs is None else pairs + part
        same = lax.broadcasted_iota(jnp.int32, pairs.shape, 0) == lax.broadcasted_iota(
            jnp.int32, pairs.shape, 1
        )
        lap_high, lap_low = split(jnp.where(same, -2.0 * pairs, pairs))
        lap[:, 0:padded] = lap_high
        lap[:, padded:] = lap_low

    def flat(ref):
        return jnp.concatenate([ref[:, m, :] for m in range(slots)], axis=1)

    base = flat(base_ref)
    base_x = base[0:1] - ix * rows_x
    base_y = base[1:2] - iy * pops_out.shape[2]
    base_z = base[2:3]
    live = jnp.concatenate(
        [jnp.full((1, padded), occ_ref[m].astype(jnp.float32)) for m in range(slots)], axis=1
    )
    scale = live * jnp.concatenate(
        [jnp.full((1, padded), stiff_ref[m]) for m in range(slots)], axis=1
    )
    lane = lax.broadcasted_iota(jnp.int32, scale.shape, 1)
    scale = jnp.where((lane // CHUNK) % 2 == 1, -scale, scale)
    off[...] = flat(offset_ref)
    sub = lax.broadcasted_iota(jnp.int32, (8, depth), 0)
    distances = ((8, base_x, 0), (16, base_y, 8), (depth, base_z, 24))

    for rows, base_row, start in distances:
        d = distance(rows, base_row)
        fits = [
            jnp.where(d < 4, 0.25, 0.0),
            jnp.where(d == 1, 1.0, jnp.where(d == 3, -1.0, 0.0)),
            jnp.where(d == 2, 1.0, jnp.where(d == 0, -1.0, 0.0)),
        ]
        for k in range(3):
            if rows == depth:
                masks_z[k] = fits[k].astype(jnp.bfloat16)
            else:
                masks[k, start : start + rows, :] = fits[k]

    def place(stage, d):
        start = stage_sizes(rows_x, stage)[0]
        sizes = stage_sizes(rows_x, stage)[1]
        return start + sum(sizes[:d]), sizes[d]

    def copy(step, stage, start, size, device):
        part = pl.ds(start, size)
        return pltpu.make_async_remote_copy(
            src_ref=send_buf.at[step, part], dst_ref=recv_buf.at[step, part],
            send_sem=send_sem.at[step, stage], recv_sem=recv_sem.at[step, stage],
            device_id=device, device_id_type=MESH,
        )

    def whole(step, stage):
        start, sizes = stage_sizes(rows_x, stage)
        return copy(step, stage, start, sum(sizes), peer[0])

    def put(step, stage, d, k, tile):
        send_buf[step, place(stage, d)[0] + k] = tile

    def got(step, stage, d, k):
        return recv_buf[step, place(stage, d)[0] + k]

    def launch(step, stage):
        sends = [copy(step, stage, *place(stage, d), peer[d]) for d in range(8)]

        @pl.when(iy % 2 == 1)
        def _():
            for d in (4, 6, 2, 5, 7, 3, 0, 1):
                sends[d].start()

        @pl.when(iy % 2 == 0)
        def _():
            for d in (5, 7, 3, 4, 6, 2, 0, 1):
                sends[d].start()

    def arrive(step, stage):
        whole(step, stage).wait_recv()

    def finish_pops(step):
        arrive(step, 2)
        from_y = {
            sy: jnp.stack([got(step, 2, d, x) for x in range(rows_x)]) for d, sy in ((2, 1), (3, -1))
        }
        for q in range(19):
            sx, sy, _ = VELOCITIES[q]
            value = moved_ref[q]
            edge_row = sub == (0 if sy == 1 else 7)
            if sy:
                value = jnp.where(edge_row, roll(from_y[sy], -YS[sy].index(q), 1), value)
            if sx:
                side = got(step, 2, 0 if sx == 1 else 1, XS[sx].index(q))
                if sy:
                    side = jnp.where(edge_row, got(step, 2, DIRS.index((sx, sy)), 0), side)
                if sx == 1:
                    value = jnp.concatenate([side[None], value[:-1]], axis=0)
                else:
                    value = jnp.concatenate([value[1:], side[None]], axis=0)
            pops_out[q] = value

    def stacked(value):
        high = value.astype(jnp.bfloat16).astype(jnp.float32)
        return jnp.concatenate([high, value - high], axis=0).astype(jnp.bfloat16)

    def substep(step, carry, first=False):
        now = off[...]
        waves = quarter_sine(jnp.concatenate([now, now + 1.0], axis=0)) * 0.25
        table_x, table_y = [
            masks[0, start : start + rows, :]
            + waves[3 + k : 4 + k] * masks[1, start : start + rows, :]
            + waves[k : k + 1] * masks[2, start : start + rows, :]
            for k, (rows, _, start) in enumerate(distances[:2])
        ]
        coarse = jnp.floor(waves * 512.0 + 0.5) * (1.0 / 512.0)
        fine = waves - coarse
        sine, cosine, sine_low, cosine_low = [
            jnp.broadcast_to(x, (depth, vertices)).astype(jnp.bfloat16)
            for x in (coarse[2:3], coarse[5:6], fine[2:3], fine[5:6])
        ]
        deep[0:depth, :] = masks_z[0] + cosine * masks_z[1] + sine * masks_z[2]
        deep[depth:, :] = cosine_low * masks_z[1] + sine_low * masks_z[2]
        strain = now - flat(rest_ref)
        six = jnp.concatenate(
            [strain[:, m * padded : (m + 1) * padded] for m in range(slots)], axis=0
        )
        if first:
            pulled, pair = None, stacked(six)
            for cut in parts:
                shape = (padded, cut.stop - cut.start)
                ids = lax.broadcasted_iota(jnp.int32, shape, 0).astype(jnp.int16)
                hit = None
                for k in range(3):
                    corner = jnp.broadcast_to(tri_ref[k : k + 1, cut], shape).astype(jnp.int16)
                    hit = ids == corner if hit is None else hit | (ids == corner)
                one = jnp.ones(shape, jnp.bfloat16)
                incidence[:, cut] = jnp.where(hit, one, jnp.zeros(shape, jnp.bfloat16))
                summed = mm(pair, incidence[:, cut], NN)
                summed = summed[0 : 3 * slots] + summed[3 * slots :]
                ones = jnp.ones((1, summed.shape[1]), jnp.bfloat16)
                part = mm(
                    jnp.concatenate([stacked(summed), ones], axis=0), incidence[:, cut], NT
                )
                pulled = part if pulled is None else pulled + part
            count = pulled[6 * slots :]
            pulled = pulled[0 : 3 * slots] + pulled[3 * slots : 6 * slots]
            pulled = pulled - 3.0 * count * six
        else:
            pulled = mm(stacked(six), lap[...], NN)
            pulled = pulled[:, 0:padded] + pulled[:, padded:]
            pulled = pulled[0 : 3 * slots] + pulled[3 * slots :]
        force_v = scale * jnp.concatenate(
            [pulled[3 * m : 3 * m + 3] for m in range(slots)], axis=1
        )
        pulled_x = [force_v[a : a + 1] * table_x for a in range(3)]
        tiles_of = {}

        def spread_tiles(names, start):
            half, sums = 8 * len(names), [None, None]
            for c, cut in enumerate(chunks):
                for n in range(0, len(names), 2):
                    blocks = [
                        pulled_x[a][:, cut] * table_y[y : y + 1, cut] if x is None
                        else pulled_x[a][x & 7 : (x & 7) + 1, cut] * table_y[0:8, cut]
                        for x, a, y in names[n : n + 2]
                    ]
                    high, low = split(jnp.concatenate(blocks, axis=0))
                    row = start + 8 * n
                    spread[row : row + 16, cut] = high
                    spread[row + half : row + half + 16, cut] = low
                part = mm(spread[start : start + 2 * half, cut], deep[:, cut], NT)
                sums[c % 2] = part if sums[c % 2] is None else sums[c % 2] + part
            total = sums[0] - sums[1]
            total = total[:half, :depth] + total[:half, depth:] + total[half:, :depth]
            for n, name in enumerate(names):
                tiles_of[name] = total[8 * n : 8 * n + 8]

        far_y = (8, 9, 15)
        outer = [(None, a, y) for y in far_y for a in range(3)]
        outer += [(x, a, 0) for x in (rows_x, rows_x + 1, -1) for a in range(3)]
        spread_tiles(outer, 0)
        for d, (sx, sy) in enumerate(DIRS):
            across = force_planes(sx, rows_x)
            if sy == 0:
                tiles = [tiles_of[x, a, 0] for x in across for a in range(3)]
            else:
                tiles = [
                    tiles_of[None, a, y] for y in ((8, 9) if sy == 1 else (15,)) for a in range(3)
                ]
                tiles = pack(tiles, across[0] & 7, len(across))
            for k, tile in enumerate(tiles):
                put(step, 0, d, k, tile)
        if first:
            pl.semaphore_wait(barrier, len(peer))
        launch(step, 0)
        spread_tiles([(x, a, 0) for x in range(rows_x) for a in range(3)], 16 * len(outer))

        if first:
            build_laplacian()
            loads[6].wait()
            loads[7].wait()
        else:
            finish_pops(step - 1)

        walled = solid_ref[...] != 0
        density, momentum, still = settle([pops_out[q] for q in range(19)], walled)
        for q in range(19):
            pops_out[q] = still[q]
        arrive(step, 0)
        force = [[tiles_of[x, a, 0] for x in range(rows_x)] for a in range(3)]
        edge = {(y, a): None for y in (0, 1, 7) for a in range(3)}
        for d, (sx, sy) in enumerate(DIRS):
            load = lambda k, d=d: got(step, 0, d, k)
            planes_in = force_planes(sx, rows_x)
            if sy == 0:
                for k, x in enumerate(planes_in):
                    for a in range(3):
                        here = force[a][landing(x, sx, rows_x)]
                        force[a][landing(x, sx, rows_x)] = here + load(3 * k + a)
                continue
            names = [(y, a) for y in ((0, 1) if sy == 1 else (7,)) for a in range(3)]
            rows, per = len(planes_in), 8 // len(planes_in)
            sent, land = planes_in[0] & 7, landing(planes_in[0], sx, rows_x)
            mask = row_mask(land, rows, depth)
            for k, name in enumerate(names):
                tile = roll(load(k // per), land - sent - (k % per) * rows, 0)
                tile = jnp.where(mask, tile, 0.0)
                edge[name] = tile if edge[name] is None else edge[name] + tile
        for a in range(3):
            for x in range(rows_x):
                tile = jnp.where(sub == 0, roll(edge[0, a], -x, 0), 0.0)
                for y in (1, 7):
                    tile = jnp.where(sub == y, roll(edge[y, a], y - x, 0), tile)
                force[a][x] = force[a][x] + tile
        force = [jnp.stack(force[a]) for a in range(3)]

        relaxed = collide(
            density, momentum, [pops_out[q] for q in range(19)], force, walled
        )
        moved = [
            roll(roll(relaxed[q], VELOCITIES[q][2], 2), VELOCITIES[q][1], 1) for q in range(19)
        ]
        for q in range(19):
            moved_ref[q] = moved[q]
        nothing = jnp.zeros((1, 8, depth), jnp.float32)
        rho, mz = {}, {}
        for cx in (-1, 0, 1):
            for cy in (-1, 0, 1):
                members = [q for q in range(19) if VELOCITIES[q][:2] == (cx, cy)]
                pad = lambda v: jnp.concatenate(
                    [nothing] * (1 + cx) + [v] + [nothing] * (1 - cx), axis=0
                )
                rho[cx, cy] = pad(total_of([moved[q] for q in members]))
                up = [moved[q] for q in members if VELOCITIES[q][2] == 1]
                down = [moved[q] for q in members if VELOCITIES[q][2] == -1]
                if up:
                    mz[cx, cy] = pad(total_of(up) - total_of(down))
        first_row, last_row = sub == 0, sub == 7
        own = {}
        zero = jnp.zeros((rows_x + 2, 8, depth), jnp.float32)
        fields = []
        for cy in (0, 1, -1):
            dens = rho[-1, cy] + rho[0, cy] + rho[1, cy]
            deep_m = [mz[cx, cy] for cx in (-1, 0, 1) if (cx, cy) in mz]
            fields.append((
                dens, rho[1, cy] - rho[-1, cy], zero if cy == 0 else cy * dens, total_of(deep_m)
            ))
        for c in range(4):
            mid, up, down = (fields[g][c] for g in range(3))
            near = mid + jnp.where(first_row, 0.0, up) + jnp.where(last_row, 0.0, down)
            if c:
                half = 0.5 * force[c - 1]
                near = near + jnp.concatenate([nothing, half, nothing], axis=0)
            far = jnp.where(first_row, up, jnp.where(last_row, down, 0.0))
            for x in range(-1, rows_x + 1):
                own[x, c] = (near[x + 1], far[x + 1])
        for d, (sx, sy) in enumerate(DIRS):
            names = [(x, c) for x in moment_planes(sx, rows_x) for c in range(4)]
            near, far = [own[n][0] for n in names], [own[n][1] for n in names]
            if sy == 0:
                tiles = near + pack(far, 7, 2)
            elif sy == 1:
                tiles = pack([jnp.where(last_row, a, b) for a, b in zip(near, far)], 7, 2)
            else:
                tiles = pack(far, 7, 1) + pack(near, 0, 2)
            for k, tile in enumerate(tiles):
                put(step, 1, d, k, tile)
        launch(step, 1)
        for n, sx in enumerate((1, -1)):
            edge = rows_x - 1 if sx == 1 else 0
            for k, q in enumerate(XS[sx]):
                put(step, 2, n, k, moved[q][edge])
        for n, sy in enumerate((1, -1)):
            rows_kept = moved[YS[sy][0]]
            start = 0 if sy == 1 else 7
            for k, q in enumerate(YS[sy][1:], 1):
                rows_kept = jnp.where(sub == (start + k) % 8, roll(moved[q], k, 1), rows_kept)
            for x in range(rows_x):
                put(step, 2, 2 + n, x, rows_kept[x])
        for n, (sx, sy) in enumerate(DIRS[4:]):
            put(step, 2, 4 + n, 0, moved[CORNER[sx, sy]][rows_x - 1 if sx == 1 else 0])
        launch(step, 2)
        arrive(step, 1)
        reach = [x for x in range(rows_x + 2)] + [-1]
        near = {(x, c): [] for x in reach for c in range(4)}
        far = {(x, c): [] for x in reach for c in range(4)}
        for name, (a, b) in own.items():
            near[name].append(a)
            far[name].append(b)
        two, edges, one = row_mask(0, 2, depth), row_mask(7, 2, depth), row_mask(7, 1, depth)
        for d, (sx, sy) in enumerate(DIRS):
            names = [
                (landing(x, sx, rows_x), c)
                for x in moment_planes(sx, rows_x) for c in range(4)
            ]
            count = len(names)
            load = lambda k, d=d: got(step, 1, d, k)
            if sy == 0:
                a = [load(k) for k in range(count)]
                b = unpack(lambda k: load(count + k), count, 2)
                b = [jnp.where(edges, t, 0.0) for t in b]
            elif sy == 1:
                both_rows = unpack(load, count, 2)
                a = [jnp.where(first_row, t, 0.0) for t in both_rows]
                b = [jnp.where(last_row, t, 0.0) for t in both_rows]
            else:
                skip = packed(count, 1)
                a = [jnp.where(one, t, 0.0) for t in unpack(load, count, 1)]
                b = unpack(lambda k: load(skip + k), count, 2)
                b = [jnp.where(two, t, 0.0) for t in b]
            for name, p, r in zip(names, a, b):
                near[name].append(p)
                far[name].append(r)
        used = row_mask(7, 3, depth)
        count = len(reach)
        for i, x in enumerate(reach):
            inverse = 1.0 / total_of(near[x, 0])
            for a in range(3):
                wide[a, i] = total_of(near[x, a + 1]) * inverse
        speed = {}
        for x in reach:
            inverse = 1.0 / jnp.where(used, total_of(far[x, 0]), 1.0)
            for a in range(3):
                speed[x, a] = total_of(far[x, a + 1]) * inverse
        for k, y in enumerate(far_y):
            for a in range(3):
                tile = jnp.zeros((8, depth), jnp.float32)
                for x in reach:
                    tile = jnp.where(sub == (x & 7), roll(speed[x, a], x - y, 0), tile)
                wide[a, count + k] = tile
        wide_high, wide_low = split(wide[...].reshape((count + 3) * 24, depth))
        twice = jnp.concatenate([wide_high, wide_high], axis=1)
        pieces = []
        for cut in chunks:
            along = mm(twice, deep[:, cut], NN) + mm(wide_low, deep[0:depth, cut], NN)
            along = along.reshape(3, count + 3, 8, along.shape[1])
            drift = []
            for a in range(3):
                near_sum = total_of([
                    along[a, i] * table_x[x & 7 : (x & 7) + 1, cut] for i, x in enumerate(reach)
                ])
                far_sum = total_of([
                    along[a, count + k] * table_y[y : y + 1, cut] for k, y in enumerate(far_y)
                ])
                total = near_sum * table_y[0:8, cut] + far_sum * table_x[:, cut]
                drift.append(jnp.sum(total, axis=0, keepdims=True))
            pieces.append(jnp.concatenate(drift, axis=0))
        off[...] = now + live * jnp.concatenate(pieces, axis=1)
        return carry

    substep(0, 0, True)
    lax.fori_loop(1, SUBSTEPS, substep, 0)
    finish_pops(SUBSTEPS - 1)

    for m in range(slots):
        offset_out[:, m, :] = off[:, m * padded : (m + 1) * padded]

    def drain(step, carry):
        for stage in range(3):
            whole(step, stage).wait_send()
        return carry

    lax.fori_loop(0, SUBSTEPS, drain, 0)


def write_kernel(pops_ref, offset_ref, pops_out, offset_out, sem):
    copies = [
        pltpu.make_async_copy(pops_ref, pops_out, sem.at[0]),
        pltpu.make_async_copy(offset_ref, offset_out, sem.at[1]),
    ]
    for x in copies:
        x.start()
    for x in copies:
        x.wait()


def local(mesh, populations, solid, base_cell, offset, rest, stiffness, occupied, triangles):
    rows_x, rows_y, depth = populations.shape[1:]
    slots, padded = offset.shape[3:]
    assert rows_y == 8 and rows_x == 4 and depth & (depth - 1) == 0
    vertices, planes = slots * padded, rows_x + 3
    S = SUBSTEPS
    f32, bf16 = jnp.float32, jnp.bfloat16
    tile = (8, depth)
    V = lambda shape, dtype=f32: pltpu.VMEM(shape, dtype)
    small = (3, slots, padded)
    i32 = jnp.int32
    scratch = [
        V(solid.shape, i32), V(small, i32), V(small), V(small),
        pltpu.SMEM((slots,), f32), pltpu.SMEM((slots,), i32), V(triangles.shape[::-1], i32),
        V((padded, triangles.shape[0]), bf16),
        V((padded, 2 * padded), bf16), V((3, vertices)),
        V(((planes + 3) * 48, vertices), bf16), V((2 * depth, vertices), bf16),
        V((3, 24, vertices)), V((3, depth, vertices), bf16),
        V((19, rows_x) + tile), V((3, planes + 3) + tile),
    ]
    tiles = sum(stage_sizes(rows_x, 2)[1], stage_sizes(rows_x, 2)[0])
    scratch += [V((S, tiles) + tile)] * 2
    scratch += [pltpu.SemaphoreType.DMA((S, 3))] * 2
    scratch += [pltpu.SemaphoreType.DMA((8,))]
    vmem = pl.BlockSpec(memory_space=pltpu.VMEM)
    hbm = pl.BlockSpec(memory_space=pltpu.HBM)
    pops, moved = pl.pallas_call(
        functools.partial(body_kernel, mesh.shape["gx"], mesh.shape["gy"]),
        out_shape=(pltpu.VMEM(populations.shape, f32), pltpu.VMEM(small, f32)),
        in_specs=[hbm] * 8,
        out_specs=(vmem, vmem),
        scratch_shapes=scratch,
        compiler_params=pltpu.CompilerParams(
            collective_id=0, has_side_effects=True, vmem_limit_bytes=24 * 1024 * 1024
        ),
    )(*[
        pltpu.with_memory_space_constraint(x, pltpu.HBM)
        for x in (
            populations, solid, base_cell.reshape(small), offset.reshape(small),
            rest.reshape(small), stiffness.reshape(slots), occupied.reshape(slots), triangles.T,
        )
    ])
    pops, moved = pl.pallas_call(
        write_kernel,
        out_shape=(
            jax.ShapeDtypeStruct(populations.shape, f32), jax.ShapeDtypeStruct(small, f32),
        ),
        in_specs=[pl.BlockSpec(memory_space=pl.ANY)] * 2,
        out_specs=(hbm, hbm),
        scratch_shapes=[pltpu.SemaphoreType.DMA((2,))],
        compiler_params=pltpu.CompilerParams(vmem_limit_bytes=1024 * 1024),
    )(pops, moved)
    return pops, moved.reshape(offset.shape)


def solution(mesh):
    in_specs = (
        P(None, "gx", "gy", None),
        P("gx", "gy", None),
        P(None, "gx", "gy", None, None),
        P(None, "gx", "gy", None, None),
        P(None, "gx", "gy", None, None),
        P("gx", "gy", None),
        P("gx", "gy", None),
        P(),
    )
    out_specs = (P(None, "gx", "gy", None), P(None, "gx", "gy", None, None))
    return jax.shard_map(
        functools.partial(local, mesh), mesh=mesh, in_specs=in_specs, out_specs=out_specs,
        check_vma=False,
    )
```

```python
import functools
import math

import jax
import jax.numpy as jnp
from jax import lax
from jax.experimental import pallas as pl
from jax.experimental.pallas import tpu as pltpu
from jax.sharding import PartitionSpec as P

SUBSTEPS = 3
VELOCITIES = [
    (0, 0, 0), (1, 0, 0), (-1, 0, 0), (0, 1, 0), (0, -1, 0), (0, 0, 1), (0, 0, -1),
    (1, 1, 0), (-1, -1, 0), (1, -1, 0), (-1, 1, 0), (1, 0, 1), (-1, 0, -1), (1, 0, -1),
    (-1, 0, 1), (0, 1, 1), (0, -1, -1), (0, 1, -1), (0, -1, 1),
]
OPPOSITE = [0, 2, 1, 4, 3, 6, 5, 8, 7, 10, 9, 12, 11, 14, 13, 16, 15, 18, 17]
LATTICE_WEIGHTS = [1.0 / 3.0] + [1.0 / 18.0] * 6 + [1.0 / 36.0] * 12
RELAX = 0.8
CHUNK = 256
MASKS = (((0, 0.25), (1, 0.25), (2, 0.25), (3, 0.25)), ((1, 1.0), (3, -1.0)), ((2, 1.0), (0, -1.0)))
XS = {s: [q for q in range(19) if VELOCITIES[q][0] == s] for s in (1, -1)}
YS = {s: [q for q in range(19) if VELOCITIES[q][1] == s] for s in (1, -1)}
CORNER = {(v[0], v[1]): q for q, v in enumerate(VELOCITIES) if v[0] and v[1]}
DIRS = [(1, 0), (-1, 0), (0, 1), (0, -1), (1, 1), (1, -1), (-1, 1), (-1, -1)]
MESH = pl.DeviceIdType.MESH
NT = (((1,), (1,)), ((), ()))
NN = (((1,), (0,)), ((), ()))


def mm(a, b, dims):
    return lax.dot_general(a, b, dims, preferred_element_type=jnp.float32)


def split(value):
    high = value.astype(jnp.bfloat16)
    low = (value - high.astype(jnp.float32)).astype(jnp.bfloat16)
    return high, low


def quarter_sine(t):
    t = t - 4.0 * jnp.floor(t * 0.25 + 0.5)
    t = jnp.maximum(jnp.minimum(t, 2.0 - t), -2.0 - t)
    x = t * (math.pi / 2.0)
    u = x * x
    p = 1.0 / 6227020800.0
    for c in (-1.0 / 39916800.0, 1.0 / 362880.0, -1.0 / 5040.0, 1.0 / 120.0, -1.0 / 6.0, 1.0):
        p = p * u + c
    return x * p


def distance(rows, base):
    cells = lax.broadcasted_iota(jnp.int32, (rows, base.shape[1]), 0)
    return (cells - base + 1) & (rows - 1)


def moments(pops):
    density = functools.reduce(lambda a, b: a + b, pops)
    momentum = []
    for a in range(3):
        plus = [pops[q] for q in range(19) if VELOCITIES[q][a] == 1]
        minus = [pops[q] for q in range(19) if VELOCITIES[q][a] == -1]
        momentum.append(
            functools.reduce(lambda a, b: a + b, plus)
            - functools.reduce(lambda a, b: a + b, minus)
        )
    return density, momentum


def settle(pops, walled):
    density, momentum = moments(pops)
    kept = 1.0 - 1.0 / RELAX
    still = [jnp.where(walled, pops[OPPOSITE[q]], kept * pops[q]) for q in range(19)]
    return density, momentum, still


def collide(density, momentum, still, force, walled):
    inverse = 1.0 / density
    rate, keep = 1.0 / RELAX, 1.0 - 0.5 / RELAX
    n = [momentum[a] + 0.5 * force[a] for a in range(3)]
    u = [jnp.where(walled, 0.0, n[a] * inverse) for a in range(3)]
    squared = u[0] * n[0] + u[1] * n[1] + u[2] * n[2]
    working = u[0] * force[0] + u[1] * force[1] + u[2] * force[2]
    even = rate * density - (1.5 * rate) * squared - (3.0 * keep) * working
    w = LATTICE_WEIGHTS[1]
    odd = [(3.0 * rate * w) * n[a] + (3.0 * keep * w) * force[a] for a in range(3)]
    twice = [(4.5 * rate * w) * n[a] + (9.0 * keep * w) * force[a] for a in range(3)]
    even = jnp.where(walled, 0.0, even)
    odd = [jnp.where(walled, 0.0, x) for x in odd]
    axis_even, half_even = w * even, (0.5 * w) * even
    half_odd, half_twice = [0.5 * x for x in odd], [0.5 * x for x in twice]

    def dot(vector, values):
        terms = [(vector[a], values[a]) for a in range(3) if vector[a]]
        out = terms[0][1] if terms[0][0] == 1 else -terms[0][1]
        for sign, value in terms[1:]:
            out = out + value if sign == 1 else out - value
        return out

    fresh = {0: LATTICE_WEIGHTS[0] * even}
    for q in range(1, 19, 2):
        vector = VELOCITIES[q]
        diagonal = sum(abs(v) for v in vector) == 2
        push = dot(vector, half_odd if diagonal else odd)
        mid = (half_even if diagonal else axis_even) + dot(vector, u) * dot(
            vector, half_twice if diagonal else twice
        )
        fresh[q], fresh[OPPOSITE[q]] = mid + push, mid - push
    return [still[q] + fresh[q] for q in range(19)]


def roll(x, shift, axis):
    size = x.shape[axis]
    shift = shift % size
    return x if shift == 0 else pltpu.roll(x, shift, axis)


def row_mask(start, rows, depth):
    sub = lax.broadcasted_iota(jnp.int32, (8, depth), 0)
    return ((sub - start) & 7) < rows


def pack(tiles, start, rows):
    per, out = 8 // rows, []
    for g in range(0, len(tiles), per):
        acc = tiles[g]
        for k, tile in enumerate(tiles[g + 1 : g + per], 1):
            mask = row_mask(start + k * rows, rows, tile.shape[1])
            acc = jnp.where(mask, roll(tile, k * rows, 0), acc)
        out.append(acc)
    return out


def unpack(load, count, rows):
    per = 8 // rows
    return [roll(load(k // per), -(k % per) * rows, 0) for k in range(count)]


def packed(count, rows):
    return -(-count // (8 // rows))


def force_planes(sx, rows_x):
    return {1: [rows_x, rows_x + 1], -1: [-1], 0: list(range(rows_x))}[sx]


def moment_planes(sx, rows_x):
    return {1: [rows_x - 1, rows_x], -1: [-1, 0, 1], 0: list(range(-1, rows_x + 1))}[sx]


def landing(x, sx, rows_x):
    return x - sx * rows_x


def force_size(sx, sy, rows_x):
    n = 3 * len(force_planes(sx, rows_x))
    return n if sy == 0 else -(-n * (2 if sy == 1 else 1) // 8)


def moment_size(sx, sy, rows_x):
    n = 4 * len(moment_planes(sx, rows_x))
    return {0: n + packed(n, 2), 1: packed(n, 2), -1: packed(n, 1) + packed(n, 2)}[sy]


def halved(sums):
    return total_of([0.5 * x for x in sums if x is not None])


def stage_sizes(rows_x, stage):
    force = [force_size(*d, rows_x) for d in DIRS]
    moment = [moment_size(*d, rows_x) for d in DIRS]
    pops = [len(XS[1])] * 2 + [rows_x] * 2 + [1] * 4
    sizes = (force, moment, pops)
    return sum(sum(x) for x in sizes[:stage]), sizes[stage]


def total_of(parts):
    return functools.reduce(lambda a, b: a + b, parts)


def body_kernel(
    peers_x, peers_y,
    pops_hbm, solid_hbm, base_hbm, offset_hbm, rest_hbm, stiff_hbm, occ_hbm, tri_hbm,
    pops_out, offset_out,
    solid_ref, base_ref, offset_ref, rest_ref, stiff_ref, occ_ref, tri_ref,
    incidence, lap, off, spread, deep, masks, masks_z, moved_ref, wide,
    send_buf, recv_buf, send_sem, recv_sem, load_sem,
):
    rows_x = pops_out.shape[1]
    depth = pops_out.shape[3]
    slots, padded = base_ref.shape[1], base_ref.shape[2]
    vertices = slots * padded
    chunks = [slice(k, min(k + CHUNK, vertices)) for k in range(0, vertices, CHUNK)]
    ix, iy = lax.axis_index("gx"), lax.axis_index("gy")
    peer = [((ix + sx + peers_x) % peers_x, (iy + sy + peers_y) % peers_y) for sx, sy in DIRS]

    loads = [
        pltpu.make_async_copy(src, dst, load_sem.at[k])
        for k, (src, dst) in enumerate((
            (tri_hbm, tri_ref), (offset_hbm, offset_ref), (rest_hbm, rest_ref),
            (base_hbm, base_ref), (stiff_hbm, stiff_ref), (occ_hbm, occ_ref),
            (solid_hbm, solid_ref), (pops_hbm, pops_out),
        ))
    ]
    for x in loads:
        x.start()
    barrier = pltpu.get_barrier_semaphore()
    for p in peer:
        pl.semaphore_signal(barrier, inc=1, device_id=p, device_id_type=MESH)

    for x in loads[:6]:
        x.wait()
    faces = tri_ref.shape[1]
    parts = [slice(k, min(k + 256, faces)) for k in range(0, faces, 256)]

    def build_laplacian():
        sums = [None, None]
        for c, cut in enumerate(parts):
            part = mm(incidence[:, cut], incidence[:, cut], NT)
            sums[c % 2] = part if sums[c % 2] is None else sums[c % 2] + part
        pairs = halved(sums) * 2.0
        same = lax.broadcasted_iota(jnp.int32, pairs.shape, 0) == lax.broadcasted_iota(
            jnp.int32, pairs.shape, 1
        )
        lap_high, lap_low = split(jnp.where(same, -2.0 * pairs, pairs))
        lap[:, 0:padded] = lap_high
        lap[:, padded:] = -lap_low

    def flat(ref):
        return jnp.concatenate([ref[:, m, :] for m in range(slots)], axis=1)

    base = flat(base_ref)
    base_x = base[0:1] - ix * rows_x
    base_y = base[1:2] - iy * pops_out.shape[2]
    base_z = base[2:3]
    live = jnp.concatenate(
        [jnp.full((1, padded), occ_ref[m].astype(jnp.float32)) for m in range(slots)], axis=1
    )
    scale = live * jnp.concatenate(
        [jnp.full((1, padded), stiff_ref[m]) for m in range(slots)], axis=1
    )
    lane = lax.broadcasted_iota(jnp.int32, scale.shape, 1)
    scale = jnp.where((lane // CHUNK) % 2 == 1, -scale, scale)
    off[...] = flat(offset_ref)
    sub = lax.broadcasted_iota(jnp.int32, (8, depth), 0)
    distances = ((8, base_x, 0), (16, base_y, 8), (depth, base_z, 24))

    short = lambda x: jnp.broadcast_to(x, (depth, vertices)).astype(jnp.int16)
    cells = lax.broadcasted_iota(jnp.int32, (depth, vertices), 0) + 1
    d = (short(cells) - short(base_z)) & short(jnp.int32(depth - 1))
    unit = jnp.ones(d.shape, jnp.bfloat16)
    for k, pairs in enumerate(MASKS):
        value = 0.0 * unit
        for j, weight in pairs:
            value = jnp.where(d == short(jnp.int32(j)), weight * unit, value)
        masks_z[k] = value
    for rows, base_row, start in distances[:2]:
        d = distance(rows, base_row)
        fits = [
            jnp.where(d < 4, 0.25, 0.0),
            jnp.where(d == 1, 1.0, jnp.where(d == 3, -1.0, 0.0)),
            jnp.where(d == 2, 1.0, jnp.where(d == 0, -1.0, 0.0)),
        ]
        for k in range(3):
            masks[k, start : start + rows, :] = fits[k]

    def place(stage, d):
        start = stage_sizes(rows_x, stage)[0]
        sizes = stage_sizes(rows_x, stage)[1]
        return start + sum(sizes[:d]), sizes[d]

    def copy(step, stage, start, size, device):
        part = pl.ds(start, size)
        return pltpu.make_async_remote_copy(
            src_ref=send_buf.at[step, part], dst_ref=recv_buf.at[step, part],
            send_sem=send_sem.at[0], recv_sem=recv_sem.at[step, stage],
            device_id=device, device_id_type=MESH,
        )

    def whole(step, stage):
        start, sizes = stage_sizes(rows_x, stage)
        return copy(step, stage, start, sum(sizes), peer[0])

    def put(step, stage, d, k, tile):
        send_buf[step, place(stage, d)[0] + k] = tile

    def got(step, stage, d, k):
        return recv_buf[step, place(stage, d)[0] + k]

    def launch(step, stage):
        sends = [copy(step, stage, *place(stage, d), peer[d]) for d in range(8)]

        for side in (0, 1):
            for part in (0, 1):
                near = 1 if side == 0 else -1
                far = 1 if part == 1 else -1
                first = (0, -near) if side == 0 else (-near, 0)
                order = [(x, y) for y in (far, -far) for x in (*first, near)]
                order += [(-near, 0), (near, 0)]

                @pl.when((ix % 2 == side) & (iy % 2 == part))
                def _(order=order):
                    for name in order:
                        sends[DIRS.index(name)].start()

    def arrive(step, stage):
        whole(step, stage).wait_recv()

    def finish_pops(step):
        arrive(step, 2)
        from_y = {
            sy: jnp.stack([got(step, 2, d, x) for x in range(rows_x)]) for d, sy in ((2, 1), (3, -1))
        }
        for q in range(19):
            sx, sy, _ = VELOCITIES[q]
            value = moved_ref[q]
            edge_row = sub == (0 if sy == 1 else 7)
            if sy:
                value = jnp.where(edge_row, roll(from_y[sy], -YS[sy].index(q), 1), value)
            if sx:
                side = got(step, 2, 0 if sx == 1 else 1, XS[sx].index(q))
                if sy:
                    side = jnp.where(edge_row, got(step, 2, DIRS.index((sx, sy)), 0), side)
                if sx == 1:
                    value = jnp.concatenate([side[None], value[:-1]], axis=0)
                else:
                    value = jnp.concatenate([value[1:], side[None]], axis=0)
            pops_out[q] = value

    def stacked(value):
        high = value.astype(jnp.bfloat16).astype(jnp.float32)
        return jnp.concatenate([high, value - high], axis=0).astype(jnp.bfloat16)

    def substep(step, carry, first=False):
        now = off[...]
        waves = quarter_sine(jnp.concatenate([now, now + 1.0], axis=0)) * 0.25
        table_x, table_y = [
            masks[0, start : start + rows, :]
            + waves[3 + k : 4 + k] * masks[1, start : start + rows, :]
            + waves[k : k + 1] * masks[2, start : start + rows, :]
            for k, (rows, _, start) in enumerate(distances[:2])
        ]
        coarse = jnp.floor(waves * 512.0 + 0.5) * (1.0 / 512.0)
        fine = waves - coarse
        sine, cosine, sine_low, cosine_low = [
            jnp.broadcast_to(x, (depth, vertices)).astype(jnp.bfloat16)
            for x in (coarse[2:3], coarse[5:6], fine[2:3], fine[5:6])
        ]
        deep[0:depth, :] = masks_z[0] + cosine * masks_z[1] + sine * masks_z[2]
        deep[depth:, :] = cosine_low * masks_z[1] + sine_low * masks_z[2]
        strain = now - flat(rest_ref)
        six = jnp.concatenate(
            [strain[:, m * padded : (m + 1) * padded] for m in range(slots)], axis=0
        )
        if first:
            sums, pair = [None, None], stacked(six)
            for c, cut in enumerate(parts):
                shape = (padded, cut.stop - cut.start)
                ids = lax.broadcasted_iota(jnp.int32, shape, 0).astype(jnp.int16)
                hit = None
                for k in range(3):
                    corner = jnp.broadcast_to(tri_ref[k : k + 1, cut], shape).astype(jnp.int16)
                    hit = ids == corner if hit is None else hit | (ids == corner)
                one = jnp.ones(shape, jnp.bfloat16)
                incidence[:, cut] = jnp.where(hit, one, jnp.zeros(shape, jnp.bfloat16))
                summed = mm(pair, incidence[:, cut], NN)
                summed = summed[0 : 3 * slots] + summed[3 * slots :]
                ones = jnp.ones((1, summed.shape[1]), jnp.bfloat16)
                part = mm(
                    jnp.concatenate([stacked(summed), ones], axis=0), incidence[:, cut], NT
                )
                sums[c % 2] = part if sums[c % 2] is None else sums[c % 2] + part
            pulled = halved(sums) * 2.0
            count = pulled[6 * slots :]
            pulled = pulled[0 : 3 * slots] + pulled[3 * slots : 6 * slots]
            pulled = pulled - 3.0 * count * six
        else:
            both = stacked(six)
            pulled = mm(both, lap[:, 0:padded], NN) - mm(both, lap[:, padded:], NN)
            pulled = pulled[0 : 3 * slots] + pulled[3 * slots :]
        force_v = scale * jnp.concatenate(
            [pulled[3 * m : 3 * m + 3] for m in range(slots)], axis=1
        )
        pulled_x = [force_v[a : a + 1] * table_x for a in range(3)]
        tiles_of = {}

        def spread_tiles(names, start):
            half, sums = 8 * len(names), [None, None]
            for c, cut in enumerate(chunks):
                for n in range(0, len(names), 2):
                    blocks = [
                        pulled_x[a][:, cut] * table_y[y : y + 1, cut] if x is None
                        else pulled_x[a][x & 7 : (x & 7) + 1, cut] * table_y[0:8, cut]
                        for x, a, y in names[n : n + 2]
                    ]
                    high, low = split(jnp.concatenate(blocks, axis=0))
                    row = start + 8 * n
                    spread[row : row + 16, cut] = high
                    spread[row + half : row + half + 16, cut] = low
                part = mm(spread[start : start + 2 * half, cut], deep[:, cut], NT)
                sums[c % 2] = part if sums[c % 2] is None else sums[c % 2] + part
            total = sums[0] - sums[1]
            total = total[:half, :depth] + total[:half, depth:] + total[half:, :depth]
            for n, name in enumerate(names):
                tiles_of[name] = total[8 * n : 8 * n + 8]

        far_y = (8, 9, 15)
        outer = [(None, a, y) for y in far_y for a in range(3)]
        outer += [(x, a, 0) for x in (rows_x, rows_x + 1, -1) for a in range(3)]
        spread_tiles(outer, 0)
        for d, (sx, sy) in enumerate(DIRS):
            across = force_planes(sx, rows_x)
            if sy == 0:
                tiles = [tiles_of[x, a, 0] for x in across for a in range(3)]
            else:
                tiles = [
                    tiles_of[None, a, y] for y in ((8, 9) if sy == 1 else (15,)) for a in range(3)
                ]
                tiles = pack(tiles, across[0] & 7, len(across))
            for k, tile in enumerate(tiles):
                put(step, 0, d, k, tile)
        if first:
            pl.semaphore_wait(barrier, len(peer))
        launch(step, 0)
        spread_tiles([(x, a, 0) for x in range(rows_x) for a in range(3)], 16 * len(outer))

        if first:
            build_laplacian()
            loads[6].wait()
            loads[7].wait()
        else:
            finish_pops(step - 1)

        walled = solid_ref[...] != 0
        density, momentum, still = settle([pops_out[q] for q in range(19)], walled)
        for q in range(19):
            pops_out[q] = still[q]
        arrive(step, 0)
        force = [[tiles_of[x, a, 0] for x in range(rows_x)] for a in range(3)]
        edge = {(y, a): None for y in (0, 1, 7) for a in range(3)}
        for d, (sx, sy) in enumerate(DIRS):
            load = lambda k, d=d: got(step, 0, d, k)
            planes_in = force_planes(sx, rows_x)
            if sy == 0:
                for k, x in enumerate(planes_in):
                    for a in range(3):
                        here = force[a][landing(x, sx, rows_x)]
                        force[a][landing(x, sx, rows_x)] = here + load(3 * k + a)
                continue
            names = [(y, a) for y in ((0, 1) if sy == 1 else (7,)) for a in range(3)]
            rows, per = len(planes_in), 8 // len(planes_in)
            sent, land = planes_in[0] & 7, landing(planes_in[0], sx, rows_x)
            mask = row_mask(land, rows, depth)
            for k, name in enumerate(names):
                tile = roll(load(k // per), land - sent - (k % per) * rows, 0)
                tile = jnp.where(mask, tile, 0.0)
                edge[name] = tile if edge[name] is None else edge[name] + tile
        for a in range(3):
            for x in range(rows_x):
                tile = jnp.where(sub == 0, roll(edge[0, a], -x, 0), 0.0)
                for y in (1, 7):
                    tile = jnp.where(sub == y, roll(edge[y, a], y - x, 0), tile)
                force[a][x] = force[a][x] + tile
        force = [jnp.stack(force[a]) for a in range(3)]

        relaxed = collide(
            density, momentum, [pops_out[q] for q in range(19)], force, walled
        )
        moved = [
            roll(roll(relaxed[q], VELOCITIES[q][2], 2), VELOCITIES[q][1], 1) for q in range(19)
        ]
        for q in range(19):
            moved_ref[q] = moved[q]
        nothing = jnp.zeros((1, 8, depth), jnp.float32)
        rho, mz = {}, {}
        for cx in (-1, 0, 1):
            for cy in (-1, 0, 1):
                members = [q for q in range(19) if VELOCITIES[q][:2] == (cx, cy)]
                pad = lambda v: jnp.concatenate(
                    [nothing] * (1 + cx) + [v] + [nothing] * (1 - cx), axis=0
                )
                rho[cx, cy] = pad(total_of([moved[q] for q in members]))
                up = [moved[q] for q in members if VELOCITIES[q][2] == 1]
                down = [moved[q] for q in members if VELOCITIES[q][2] == -1]
                if up:
                    mz[cx, cy] = pad(total_of(up) - total_of(down))
        first_row, last_row = sub == 0, sub == 7
        own = {}
        zero = jnp.zeros((rows_x + 2, 8, depth), jnp.float32)
        fields = []
        for cy in (0, 1, -1):
            dens = rho[-1, cy] + rho[0, cy] + rho[1, cy]
            deep_m = [mz[cx, cy] for cx in (-1, 0, 1) if (cx, cy) in mz]
            fields.append((
                dens, rho[1, cy] - rho[-1, cy], zero if cy == 0 else cy * dens, total_of(deep_m)
            ))
        for c in range(4):
            mid, up, down = (fields[g][c] for g in range(3))
            near = mid + jnp.where(first_row, 0.0, up) + jnp.where(last_row, 0.0, down)
            if c:
                half = 0.5 * force[c - 1]
                near = near + jnp.concatenate([nothing, half, nothing], axis=0)
            far = jnp.where(first_row, up, jnp.where(last_row, down, 0.0))
            for x in range(-1, rows_x + 1):
                own[x, c] = (near[x + 1], far[x + 1])
        for d, (sx, sy) in enumerate(DIRS):
            names = [(x, c) for x in moment_planes(sx, rows_x) for c in range(4)]
            near, far = [own[n][0] for n in names], [own[n][1] for n in names]
            if sy == 0:
                tiles = near + pack(far, 7, 2)
            elif sy == 1:
                tiles = pack([jnp.where(last_row, a, b) for a, b in zip(near, far)], 7, 2)
            else:
                tiles = pack(far, 7, 1) + pack(near, 0, 2)
            for k, tile in enumerate(tiles):
                put(step, 1, d, k, tile)
        launch(step, 1)
        for n, sx in enumerate((1, -1)):
            edge = rows_x - 1 if sx == 1 else 0
            for k, q in enumerate(XS[sx]):
                put(step, 2, n, k, moved[q][edge])
        for n, sy in enumerate((1, -1)):
            rows_kept = moved[YS[sy][0]]
            start = 0 if sy == 1 else 7
            for k, q in enumerate(YS[sy][1:], 1):
                rows_kept = jnp.where(sub == (start + k) % 8, roll(moved[q], k, 1), rows_kept)
            for x in range(rows_x):
                put(step, 2, 2 + n, x, rows_kept[x])
        for n, (sx, sy) in enumerate(DIRS[4:]):
            put(step, 2, 4 + n, 0, moved[CORNER[sx, sy]][rows_x - 1 if sx == 1 else 0])
        launch(step, 2)
        arrive(step, 1)
        reach = [x for x in range(rows_x + 2)] + [-1]
        near = {(x, c): [] for x in reach for c in range(4)}
        far = {(x, c): [] for x in reach for c in range(4)}
        for name, (a, b) in own.items():
            near[name].append(a)
            far[name].append(b)
        two, edges, one = row_mask(0, 2, depth), row_mask(7, 2, depth), row_mask(7, 1, depth)
        for d, (sx, sy) in enumerate(DIRS):
            names = [
                (landing(x, sx, rows_x), c)
                for x in moment_planes(sx, rows_x) for c in range(4)
            ]
            count = len(names)
            load = lambda k, d=d: got(step, 1, d, k)
            if sy == 0:
                a = [load(k) for k in range(count)]
                b = unpack(lambda k: load(count + k), count, 2)
                b = [jnp.where(edges, t, 0.0) for t in b]
            elif sy == 1:
                both_rows = unpack(load, count, 2)
                a = [jnp.where(first_row, t, 0.0) for t in both_rows]
                b = [jnp.where(last_row, t, 0.0) for t in both_rows]
            else:
                skip = packed(count, 1)
                a = [jnp.where(one, t, 0.0) for t in unpack(load, count, 1)]
                b = unpack(lambda k: load(skip + k), count, 2)
                b = [jnp.where(two, t, 0.0) for t in b]
            for name, p, r in zip(names, a, b):
                near[name].append(p)
                far[name].append(r)
        used = row_mask(7, 3, depth)
        count = len(reach)
        for i, x in enumerate(reach):
            inverse = 1.0 / total_of(near[x, 0])
            for a in range(3):
                wide[a, i] = total_of(near[x, a + 1]) * inverse
        speed = {}
        for x in reach:
            inverse = 1.0 / jnp.where(used, total_of(far[x, 0]), 1.0)
            for a in range(3):
                speed[x, a] = total_of(far[x, a + 1]) * inverse
        for k, y in enumerate(far_y):
            for a in range(3):
                tile = jnp.zeros((8, depth), jnp.float32)
                for x in reach:
                    tile = jnp.where(sub == (x & 7), roll(speed[x, a], x - y, 0), tile)
                wide[a, count + k] = tile
        wide_high, wide_low = split(wide[...].reshape((count + 3) * 24, depth))
        twice = jnp.concatenate([wide_high, wide_high], axis=1)
        pieces = []
        for cut in chunks:
            along = mm(twice, deep[:, cut], NN) + mm(wide_low, deep[0:depth, cut], NN)
            along = along.reshape(3, count + 3, 8, along.shape[1])
            drift = []
            for a in range(3):
                near_sum = total_of([
                    along[a, i] * table_x[x & 7 : (x & 7) + 1, cut] for i, x in enumerate(reach)
                ])
                far_sum = total_of([
                    along[a, count + k] * table_y[y : y + 1, cut] for k, y in enumerate(far_y)
                ])
                total = near_sum * table_y[0:8, cut] + far_sum * table_x[:, cut]
                drift.append(jnp.sum(total, axis=0, keepdims=True))
            pieces.append(jnp.concatenate(drift, axis=0))
        off[...] = now + live * jnp.concatenate(pieces, axis=1)
        return carry

    substep(0, 0, True)
    lax.fori_loop(1, SUBSTEPS, substep, 0)
    finish_pops(SUBSTEPS - 1)

    for m in range(slots):
        offset_out[:, m, :] = off[:, m * padded : (m + 1) * padded]

    pltpu.make_async_remote_copy(
        src_ref=send_buf, dst_ref=recv_buf, send_sem=send_sem.at[0], recv_sem=recv_sem.at[0, 0],
        device_id=peer[0], device_id_type=MESH,
    ).wait_send()


def write_kernel(pops_ref, offset_ref, pops_out, offset_out, sem):
    copies = [
        pltpu.make_async_copy(pops_ref, pops_out, sem.at[0]),
        pltpu.make_async_copy(offset_ref, offset_out, sem.at[1]),
    ]
    for x in copies:
        x.start()
    for x in copies:
        x.wait()


def local(mesh, populations, solid, base_cell, offset, rest, stiffness, occupied, triangles):
    rows_x, rows_y, depth = populations.shape[1:]
    slots, padded = offset.shape[3:]
    assert rows_y == 8 and rows_x == 4 and depth & (depth - 1) == 0
    vertices, planes = slots * padded, rows_x + 3
    S = SUBSTEPS
    f32, bf16 = jnp.float32, jnp.bfloat16
    tile = (8, depth)
    V = lambda shape, dtype=f32: pltpu.VMEM(shape, dtype)
    small = (3, slots, padded)
    i32 = jnp.int32
    scratch = [
        V(solid.shape, i32), V(small, i32), V(small), V(small),
        pltpu.SMEM((slots,), f32), pltpu.SMEM((slots,), i32), V(triangles.shape[::-1], i32),
        V((padded, triangles.shape[0]), bf16),
        V((padded, 2 * padded), bf16), V((3, vertices)),
        V(((planes + 3) * 48, vertices), bf16), V((2 * depth, vertices), bf16),
        V((3, 24, vertices)), V((3, depth, vertices), bf16),
        V((19, rows_x) + tile), V((3, planes + 3) + tile),
    ]
    tiles = sum(stage_sizes(rows_x, 2)[1], stage_sizes(rows_x, 2)[0])
    scratch += [V((S, tiles) + tile)] * 2
    scratch += [pltpu.SemaphoreType.DMA((1,)), pltpu.SemaphoreType.DMA((S, 3))]
    scratch += [pltpu.SemaphoreType.DMA((8,))]
    vmem = pl.BlockSpec(memory_space=pltpu.VMEM)
    hbm = pl.BlockSpec(memory_space=pltpu.HBM)
    pops, moved = pl.pallas_call(
        functools.partial(body_kernel, mesh.shape["gx"], mesh.shape["gy"]),
        out_shape=(pltpu.VMEM(populations.shape, f32), pltpu.VMEM(small, f32)),
        in_specs=[hbm] * 8,
        out_specs=(vmem, vmem),
        scratch_shapes=scratch,
        compiler_params=pltpu.CompilerParams(
            collective_id=0, has_side_effects=True, vmem_limit_bytes=24 * 1024 * 1024
        ),
    )(*[
        pltpu.with_memory_space_constraint(x, pltpu.HBM)
        for x in (
            populations, solid, base_cell.reshape(small), offset.reshape(small),
            rest.reshape(small), stiffness.reshape(slots), occupied.reshape(slots), triangles.T,
        )
    ])
    pops, moved = pl.pallas_call(
        write_kernel,
        out_shape=(
            jax.ShapeDtypeStruct(populations.shape, f32), jax.ShapeDtypeStruct(small, f32),
        ),
        in_specs=[pl.BlockSpec(memory_space=pl.ANY)] * 2,
        out_specs=(hbm, hbm),
        scratch_shapes=[pltpu.SemaphoreType.DMA((2,))],
        compiler_params=pltpu.CompilerParams(vmem_limit_bytes=1024 * 1024),
    )(pops, moved)
    return pops, moved.reshape(offset.shape)


def solution(mesh):
    in_specs = (
        P(None, "gx", "gy", None),
        P("gx", "gy", None),
        P(None, "gx", "gy", None, None),
        P(None, "gx", "gy", None, None),
        P(None, "gx", "gy", None, None),
        P("gx", "gy", None),
        P("gx", "gy", None),
        P(),
    )
    out_specs = (P(None, "gx", "gy", None), P(None, "gx", "gy", None, None))
    return jax.shard_map(
        functools.partial(local, mesh), mesh=mesh, in_specs=in_specs, out_specs=out_specs,
        check_vma=False,
    )
```

```python
import functools
import math

import jax
import jax.numpy as jnp
from jax import lax
from jax.experimental import pallas as pl
from jax.experimental.pallas import tpu as pltpu
from jax.sharding import PartitionSpec as P

SUBSTEPS = 3
VELOCITIES = [
    (0, 0, 0), (1, 0, 0), (-1, 0, 0), (0, 1, 0), (0, -1, 0), (0, 0, 1), (0, 0, -1),
    (1, 1, 0), (-1, -1, 0), (1, -1, 0), (-1, 1, 0), (1, 0, 1), (-1, 0, -1), (1, 0, -1),
    (-1, 0, 1), (0, 1, 1), (0, -1, -1), (0, 1, -1), (0, -1, 1),
]
OPPOSITE = [0, 2, 1, 4, 3, 6, 5, 8, 7, 10, 9, 12, 11, 14, 13, 16, 15, 18, 17]
LATTICE_WEIGHTS = [1.0 / 3.0] + [1.0 / 18.0] * 6 + [1.0 / 36.0] * 12
RELAX = 0.8
CHUNK = 256
MASKS = (((0, 0.25), (1, 0.25), (2, 0.25), (3, 0.25)), ((1, 1.0), (3, -1.0)), ((2, 1.0), (0, -1.0)))
XS = {s: [q for q in range(19) if VELOCITIES[q][0] == s] for s in (1, -1)}
YS = {s: [q for q in range(19) if VELOCITIES[q][1] == s] for s in (1, -1)}
CORNER = {(v[0], v[1]): q for q, v in enumerate(VELOCITIES) if v[0] and v[1]}
DIRS = [(1, 0), (-1, 0), (0, 1), (0, -1), (1, 1), (1, -1), (-1, 1), (-1, -1)]
MESH = pl.DeviceIdType.MESH
NT = (((1,), (1,)), ((), ()))
NN = (((1,), (0,)), ((), ()))


def mm(a, b, dims):
    return lax.dot_general(a, b, dims, preferred_element_type=jnp.float32)


def split(value):
    high = value.astype(jnp.bfloat16)
    low = (value - high.astype(jnp.float32)).astype(jnp.bfloat16)
    return high, low


def quarter_sine(t):
    t = t - 4.0 * jnp.floor(t * 0.25 + 0.5)
    t = jnp.maximum(jnp.minimum(t, 2.0 - t), -2.0 - t)
    x = t * (math.pi / 2.0)
    u = x * x
    p = 1.0 / 6227020800.0
    for c in (-1.0 / 39916800.0, 1.0 / 362880.0, -1.0 / 5040.0, 1.0 / 120.0, -1.0 / 6.0, 1.0):
        p = p * u + c
    return x * p


def distance(rows, base):
    cells = lax.broadcasted_iota(jnp.int32, (rows, base.shape[1]), 0)
    return (cells - base + 1) & (rows - 1)


def moments(pops):
    density = functools.reduce(lambda a, b: a + b, pops)
    momentum = []
    for a in range(3):
        plus = [pops[q] for q in range(19) if VELOCITIES[q][a] == 1]
        minus = [pops[q] for q in range(19) if VELOCITIES[q][a] == -1]
        momentum.append(
            functools.reduce(lambda a, b: a + b, plus)
            - functools.reduce(lambda a, b: a + b, minus)
        )
    return density, momentum


def settle(pops, walled):
    density, momentum = moments(pops)
    kept = 1.0 - 1.0 / RELAX
    still = [jnp.where(walled, pops[OPPOSITE[q]], kept * pops[q]) for q in range(19)]
    return density, momentum, still


def collide(density, momentum, still, force, walled):
    inverse = 1.0 / density
    rate, keep = 1.0 / RELAX, 1.0 - 0.5 / RELAX
    n = [momentum[a] + 0.5 * force[a] for a in range(3)]
    u = [jnp.where(walled, 0.0, n[a] * inverse) for a in range(3)]
    squared = u[0] * n[0] + u[1] * n[1] + u[2] * n[2]
    working = u[0] * force[0] + u[1] * force[1] + u[2] * force[2]
    even = rate * density - (1.5 * rate) * squared - (3.0 * keep) * working
    w = LATTICE_WEIGHTS[1]
    odd = [(3.0 * rate * w) * n[a] + (3.0 * keep * w) * force[a] for a in range(3)]
    twice = [(4.5 * rate * w) * n[a] + (9.0 * keep * w) * force[a] for a in range(3)]
    even = jnp.where(walled, 0.0, even)
    odd = [jnp.where(walled, 0.0, x) for x in odd]
    axis_even, half_even = w * even, (0.5 * w) * even
    half_odd, half_twice = [0.5 * x for x in odd], [0.5 * x for x in twice]

    def dot(vector, values):
        terms = [(vector[a], values[a]) for a in range(3) if vector[a]]
        out = terms[0][1] if terms[0][0] == 1 else -terms[0][1]
        for sign, value in terms[1:]:
            out = out + value if sign == 1 else out - value
        return out

    fresh = {0: LATTICE_WEIGHTS[0] * even}
    for q in range(1, 19, 2):
        vector = VELOCITIES[q]
        diagonal = sum(abs(v) for v in vector) == 2
        push = dot(vector, half_odd if diagonal else odd)
        mid = (half_even if diagonal else axis_even) + dot(vector, u) * dot(
            vector, half_twice if diagonal else twice
        )
        fresh[q], fresh[OPPOSITE[q]] = mid + push, mid - push
    return [still[q] + fresh[q] for q in range(19)]


def roll(x, shift, axis):
    size = x.shape[axis]
    shift = shift % size
    return x if shift == 0 else pltpu.roll(x, shift, axis)


def row_mask(start, rows, depth):
    sub = lax.broadcasted_iota(jnp.int32, (8, depth), 0)
    return ((sub - start) & 7) < rows


def pack(tiles, start, rows):
    per, out = 8 // rows, []
    for g in range(0, len(tiles), per):
        acc = tiles[g]
        for k, tile in enumerate(tiles[g + 1 : g + per], 1):
            mask = row_mask(start + k * rows, rows, tile.shape[1])
            acc = jnp.where(mask, roll(tile, k * rows, 0), acc)
        out.append(acc)
    return out


def unpack(load, count, rows):
    per = 8 // rows
    return [roll(load(k // per), -(k % per) * rows, 0) for k in range(count)]


def packed(count, rows):
    return -(-count // (8 // rows))


def force_planes(sx, rows_x):
    return {1: [rows_x, rows_x + 1], -1: [-1], 0: list(range(rows_x))}[sx]


def moment_planes(sx, rows_x):
    return {1: [rows_x - 1, rows_x], -1: [-1, 0, 1], 0: list(range(-1, rows_x + 1))}[sx]


def landing(x, sx, rows_x):
    return x - sx * rows_x


def force_size(sx, sy, rows_x):
    n = 3 * len(force_planes(sx, rows_x))
    return n if sy == 0 else -(-n * (2 if sy == 1 else 1) // 8)


def moment_names(sx, sy, rows_x, beyond):
    names = []
    for x in moment_planes(sx, rows_x):
        ring = x in (-1, rows_x)
        if beyond and sy == -1:
            names += [(x, c) for c in ((0,) if ring else (0, 1, 3))]
        else:
            names += [(x, c) for c in ((0, 2, 3) if ring else (0, 1, 2, 3))]
    return names


def restore(part, sx, sy, rows_x):
    for x in moment_planes(sx, rows_x):
        ring = {-1: -1.0, rows_x: 1.0}.get(x)
        if (x, 1) not in part:
            part[x, 1] = ring * part[x, 0]
        if (x, 2) not in part:
            part[x, 2] = float(sy) * part[x, 0]
    return part


def moment_size(sx, sy, rows_x):
    near, far = (len(moment_names(sx, sy, rows_x, k)) for k in (False, True))
    return {0: near + packed(far, 2), 1: packed(near, 2), -1: packed(far, 1) + packed(near, 2)}[sy]


def halved(sums):
    return total_of([0.5 * x for x in sums if x is not None])


def stage_sizes(rows_x, stage):
    force = [force_size(*d, rows_x) for d in DIRS]
    moment = [moment_size(*d, rows_x) for d in DIRS]
    pops = [len(XS[1])] * 2 + [rows_x] * 2 + [1] * 4
    sizes = (force, moment, pops)
    return sum(sum(x) for x in sizes[:stage]), sizes[stage]


def total_of(parts):
    return functools.reduce(lambda a, b: a + b, parts)


def body_kernel(
    peers_x, peers_y,
    pops_hbm, solid_hbm, base_hbm, offset_hbm, rest_hbm, stiff_hbm, occ_hbm, tri_hbm,
    pops_out, offset_out,
    solid_ref, base_ref, offset_ref, rest_ref, stiff_ref, occ_ref, tri_ref,
    incidence, lap, off, spread, deep, masks, masks_z, moved_ref, wide,
    send_buf, recv_buf, send_sem, recv_sem, load_sem,
):
    rows_x = pops_out.shape[1]
    depth = pops_out.shape[3]
    slots, padded = base_ref.shape[1], base_ref.shape[2]
    vertices = slots * padded
    chunks = [slice(k, min(k + CHUNK, vertices)) for k in range(0, vertices, CHUNK)]
    ix, iy = lax.axis_index("gx"), lax.axis_index("gy")
    peer = [((ix + sx + peers_x) % peers_x, (iy + sy + peers_y) % peers_y) for sx, sy in DIRS]

    loads = [
        pltpu.make_async_copy(src, dst, load_sem.at[k])
        for k, (src, dst) in enumerate((
            (tri_hbm, tri_ref), (offset_hbm, offset_ref), (rest_hbm, rest_ref),
            (base_hbm, base_ref), (stiff_hbm, stiff_ref), (occ_hbm, occ_ref),
            (solid_hbm, solid_ref), (pops_hbm, pops_out),
        ))
    ]
    for x in loads:
        x.start()
    barrier = pltpu.get_barrier_semaphore()
    for p in peer:
        pl.semaphore_signal(barrier, inc=1, device_id=p, device_id_type=MESH)

    for x in loads[:6]:
        x.wait()
    faces = tri_ref.shape[1]
    parts = [slice(k, min(k + 256, faces)) for k in range(0, faces, 256)]

    def build_laplacian():
        sums = [None, None]
        for c, cut in enumerate(parts):
            part = mm(incidence[:, cut], incidence[:, cut], NT)
            sums[c % 2] = part if sums[c % 2] is None else sums[c % 2] + part
        pairs = halved(sums) * 2.0
        same = lax.broadcasted_iota(jnp.int32, pairs.shape, 0) == lax.broadcasted_iota(
            jnp.int32, pairs.shape, 1
        )
        lap_high, lap_low = split(jnp.where(same, -2.0 * pairs, pairs))
        lap[:, 0:padded] = lap_high
        lap[:, padded:] = -lap_low

    def flat(ref):
        return jnp.concatenate([ref[:, m, :] for m in range(slots)], axis=1)

    base = flat(base_ref)
    base_x = base[0:1] - ix * rows_x
    base_y = base[1:2] - iy * pops_out.shape[2]
    base_z = base[2:3]
    live = jnp.concatenate(
        [jnp.full((1, padded), occ_ref[m].astype(jnp.float32)) for m in range(slots)], axis=1
    )
    scale = live * jnp.concatenate(
        [jnp.full((1, padded), stiff_ref[m]) for m in range(slots)], axis=1
    )
    lane = lax.broadcasted_iota(jnp.int32, scale.shape, 1)
    scale = jnp.where((lane // CHUNK) % 2 == 1, -scale, scale)
    off[...] = flat(offset_ref)
    sub = lax.broadcasted_iota(jnp.int32, (8, depth), 0)
    distances = ((8, base_x, 0), (16, base_y, 8), (depth, base_z, 24))

    short = lambda x: jnp.broadcast_to(x, (depth, vertices)).astype(jnp.int16)
    cells = lax.broadcasted_iota(jnp.int32, (depth, vertices), 0) + 1
    d = (short(cells) - short(base_z)) & short(jnp.int32(depth - 1))
    unit = jnp.ones(d.shape, jnp.bfloat16)
    for k, pairs in enumerate(MASKS):
        value = 0.0 * unit
        for j, weight in pairs:
            value = jnp.where(d == short(jnp.int32(j)), weight * unit, value)
        masks_z[k] = value
    for rows, base_row, start in distances[:2]:
        d = distance(rows, base_row)
        fits = [
            jnp.where(d < 4, 0.25, 0.0),
            jnp.where(d == 1, 1.0, jnp.where(d == 3, -1.0, 0.0)),
            jnp.where(d == 2, 1.0, jnp.where(d == 0, -1.0, 0.0)),
        ]
        for k in range(3):
            masks[k, start : start + rows, :] = fits[k]

    def place(stage, d):
        start = stage_sizes(rows_x, stage)[0]
        sizes = stage_sizes(rows_x, stage)[1]
        return start + sum(sizes[:d]), sizes[d]

    def copy(step, stage, start, size, device):
        part = pl.ds(start, size)
        return pltpu.make_async_remote_copy(
            src_ref=send_buf.at[step, part], dst_ref=recv_buf.at[step, part],
            send_sem=send_sem.at[0], recv_sem=recv_sem.at[step, stage],
            device_id=device, device_id_type=MESH,
        )

    def whole(step, stage):
        start, sizes = stage_sizes(rows_x, stage)
        return copy(step, stage, start, sum(sizes), peer[0])

    def put(step, stage, d, k, tile):
        send_buf[step, place(stage, d)[0] + k] = tile

    def got(step, stage, d, k):
        return recv_buf[step, place(stage, d)[0] + k]

    def launch_far(step, stage):
        sends = {DIRS[d]: copy(step, stage, *place(stage, d), peer[d]) for d in range(2, 8)}
        for side in (0, 1):
            for part in (0, 1):
                near = 1 if side == 0 else -1
                far = 1 if part == 1 else -1
                turn = (0, -near, near) if side == 0 else (-near, near, 0)
                order = [(x, y) for y in (far, -far) for x in turn]

                @pl.when((ix % 2 == side) & (iy % 2 == part))
                def _(order=order):
                    for name in order:
                        sends[name].start()

    def launch_near(step, stage):
        for d in (1, 0):
            copy(step, stage, *place(stage, d), peer[d]).start()

    def arrive(step, stage):
        whole(step, stage).wait_recv()

    def finish_pops(step):
        arrive(step, 2)
        from_y = {
            sy: jnp.stack([got(step, 2, d, x) for x in range(rows_x)]) for d, sy in ((2, 1), (3, -1))
        }
        for q in range(19):
            sx, sy, _ = VELOCITIES[q]
            value = moved_ref[q]
            edge_row = sub == (0 if sy == 1 else 7)
            if sy:
                value = jnp.where(edge_row, roll(from_y[sy], -YS[sy].index(q), 1), value)
            if sx:
                side = got(step, 2, 0 if sx == 1 else 1, XS[sx].index(q))
                if sy:
                    side = jnp.where(edge_row, got(step, 2, DIRS.index((sx, sy)), 0), side)
                if sx == 1:
                    value = jnp.concatenate([side[None], value[:-1]], axis=0)
                else:
                    value = jnp.concatenate([value[1:], side[None]], axis=0)
            pops_out[q] = value

    def stacked(value):
        high = value.astype(jnp.bfloat16).astype(jnp.float32)
        return jnp.concatenate([high, value - high], axis=0).astype(jnp.bfloat16)

    def substep(step, carry, first=False):
        now = off[...]
        waves = quarter_sine(jnp.concatenate([now, now + 1.0], axis=0)) * 0.25
        table_x, table_y = [
            masks[0, start : start + rows, :]
            + waves[3 + k : 4 + k] * masks[1, start : start + rows, :]
            + waves[k : k + 1] * masks[2, start : start + rows, :]
            for k, (rows, _, start) in enumerate(distances[:2])
        ]
        coarse = jnp.floor(waves * 512.0 + 0.5) * (1.0 / 512.0)
        fine = waves - coarse
        sine, cosine, sine_low, cosine_low = [
            jnp.broadcast_to(x, (depth, vertices)).astype(jnp.bfloat16)
            for x in (coarse[2:3], coarse[5:6], fine[2:3], fine[5:6])
        ]
        deep[0:depth, :] = masks_z[0] + cosine * masks_z[1] + sine * masks_z[2]
        deep[depth:, :] = cosine_low * masks_z[1] + sine_low * masks_z[2]
        strain = now - flat(rest_ref)
        six = jnp.concatenate(
            [strain[:, m * padded : (m + 1) * padded] for m in range(slots)], axis=0
        )
        if first:
            sums, pair = [None, None], stacked(six)
            for c, cut in enumerate(parts):
                shape = (padded, cut.stop - cut.start)
                ids = lax.broadcasted_iota(jnp.int32, shape, 0).astype(jnp.int16)
                hit = None
                for k in range(3):
                    corner = jnp.broadcast_to(tri_ref[k : k + 1, cut], shape).astype(jnp.int16)
                    hit = ids == corner if hit is None else hit | (ids == corner)
                one = jnp.ones(shape, jnp.bfloat16)
                incidence[:, cut] = jnp.where(hit, one, jnp.zeros(shape, jnp.bfloat16))
                summed = mm(pair, incidence[:, cut], NN)
                summed = summed[0 : 3 * slots] + summed[3 * slots :]
                ones = jnp.ones((1, summed.shape[1]), jnp.bfloat16)
                part = mm(
                    jnp.concatenate([stacked(summed), ones], axis=0), incidence[:, cut], NT
                )
                sums[c % 2] = part if sums[c % 2] is None else sums[c % 2] + part
            pulled = halved(sums) * 2.0
            count = pulled[6 * slots :]
            pulled = pulled[0 : 3 * slots] + pulled[3 * slots : 6 * slots]
            pulled = pulled - 3.0 * count * six
        else:
            both = stacked(six)
            pulled = mm(both, lap[:, 0:padded], NN) - mm(both, lap[:, padded:], NN)
            pulled = pulled[0 : 3 * slots] + pulled[3 * slots :]
        force_v = scale * jnp.concatenate(
            [pulled[3 * m : 3 * m + 3] for m in range(slots)], axis=1
        )
        pulled_x = [force_v[a : a + 1] * table_x for a in range(3)]
        tiles_of = {}

        def spread_tiles(names, start):
            half, sums = 16 * -(-len(names) // 2), [None, None]
            for c, cut in enumerate(chunks):
                for n in range(0, len(names), 2):
                    blocks = [
                        pulled_x[a][:, cut] * table_y[y : y + 1, cut] if x is None
                        else pulled_x[a][x & 7 : (x & 7) + 1, cut] * table_y[0:8, cut]
                        for x, a, y in names[n : n + 2]
                    ]
                    if len(blocks) == 1:
                        blocks = blocks * 2
                    high, low = split(jnp.concatenate(blocks, axis=0))
                    row = start + 8 * n
                    spread[row : row + 16, cut] = high
                    spread[row + half : row + half + 16, cut] = low
                part = mm(spread[start : start + 2 * half, cut], deep[:, cut], NT)
                sums[c % 2] = part if sums[c % 2] is None else sums[c % 2] + part
            total = sums[0] - sums[1]
            total = total[:half, :depth] + total[:half, depth:] + total[half:, :depth]
            for n, name in enumerate(names):
                tiles_of[name] = total[8 * n : 8 * n + 8]

        far_y = (8, 9, 15)
        outer = [(None, a, y) for y in far_y for a in range(3)]
        outer += [(x, a, 0) for x in (rows_x, rows_x + 1, -1) for a in range(3)]
        spread_tiles(outer, 0)
        def put_force(d):
            sx, sy = DIRS[d]
            across = force_planes(sx, rows_x)
            if sy == 0:
                tiles = [tiles_of[x, a, 0] for x in across for a in range(3)]
            else:
                tiles = [
                    tiles_of[None, a, y] for y in ((8, 9) if sy == 1 else (15,)) for a in range(3)
                ]
                tiles = pack(tiles, across[0] & 7, len(across))
            for k, tile in enumerate(tiles):
                put(step, 0, d, k, tile)

        for d in range(8):
            put_force(d)
        if first:
            pl.semaphore_wait(barrier, len(peer))
        launch_far(step, 0)
        launch_near(step, 0)
        inner = [(x, a, 0) for x in range(rows_x) for a in range(3)]
        spread_tiles(inner, 16 * len(outer))
        if first:
            build_laplacian()
            loads[6].wait()
            loads[7].wait()
        else:
            finish_pops(step - 1)

        walled = solid_ref[...] != 0
        density, momentum, still = settle([pops_out[q] for q in range(19)], walled)
        for q in range(19):
            pops_out[q] = still[q]
        arrive(step, 0)
        force = [[tiles_of[x, a, 0] for x in range(rows_x)] for a in range(3)]
        edge = {(y, a): None for y in (0, 1, 7) for a in range(3)}
        for d, (sx, sy) in enumerate(DIRS):
            load = lambda k, d=d: got(step, 0, d, k)
            planes_in = force_planes(sx, rows_x)
            if sy == 0:
                for k, x in enumerate(planes_in):
                    for a in range(3):
                        here = force[a][landing(x, sx, rows_x)]
                        force[a][landing(x, sx, rows_x)] = here + load(3 * k + a)
                continue
            names = [(y, a) for y in ((0, 1) if sy == 1 else (7,)) for a in range(3)]
            rows, per = len(planes_in), 8 // len(planes_in)
            sent, land = planes_in[0] & 7, landing(planes_in[0], sx, rows_x)
            mask = row_mask(land, rows, depth)
            for k, name in enumerate(names):
                tile = roll(load(k // per), land - sent - (k % per) * rows, 0)
                tile = jnp.where(mask, tile, 0.0)
                edge[name] = tile if edge[name] is None else edge[name] + tile
        for a in range(3):
            for x in range(rows_x):
                tile = jnp.where(sub == 0, roll(edge[0, a], -x, 0), 0.0)
                for y in (1, 7):
                    tile = jnp.where(sub == y, roll(edge[y, a], y - x, 0), tile)
                force[a][x] = force[a][x] + tile
        force = [jnp.stack(force[a]) for a in range(3)]

        relaxed = collide(
            density, momentum, [pops_out[q] for q in range(19)], force, walled
        )
        moved = [
            roll(roll(relaxed[q], VELOCITIES[q][2], 2), VELOCITIES[q][1], 1) for q in range(19)
        ]
        for q in range(19):
            moved_ref[q] = moved[q]
        nothing = jnp.zeros((1, 8, depth), jnp.float32)
        rho, mz = {}, {}
        for cx in (-1, 0, 1):
            for cy in (-1, 0, 1):
                members = [q for q in range(19) if VELOCITIES[q][:2] == (cx, cy)]
                pad = lambda v: jnp.concatenate(
                    [nothing] * (1 + cx) + [v] + [nothing] * (1 - cx), axis=0
                )
                rho[cx, cy] = pad(total_of([moved[q] for q in members]))
                up = [moved[q] for q in members if VELOCITIES[q][2] == 1]
                down = [moved[q] for q in members if VELOCITIES[q][2] == -1]
                if up:
                    mz[cx, cy] = pad(total_of(up) - total_of(down))
        first_row, last_row = sub == 0, sub == 7
        own = {}
        zero = jnp.zeros((rows_x + 2, 8, depth), jnp.float32)
        fields = []
        for cy in (0, 1, -1):
            dens = rho[-1, cy] + rho[0, cy] + rho[1, cy]
            deep_m = [mz[cx, cy] for cx in (-1, 0, 1) if (cx, cy) in mz]
            fields.append((
                dens, rho[1, cy] - rho[-1, cy], zero if cy == 0 else cy * dens, total_of(deep_m)
            ))
        for c in range(4):
            mid, up, down = (fields[g][c] for g in range(3))
            near = mid + jnp.where(first_row, 0.0, up) + jnp.where(last_row, 0.0, down)
            if c:
                half = 0.5 * force[c - 1]
                near = near + jnp.concatenate([nothing, half, nothing], axis=0)
            far = jnp.where(first_row, up, jnp.where(last_row, down, 0.0))
            for x in range(-1, rows_x + 1):
                own[x, c] = (near[x + 1], far[x + 1])
        for d in (2, 3, 4, 5, 6, 7, 0, 1):
            sx, sy = DIRS[d]
            near = [own[n][0] for n in moment_names(sx, sy, rows_x, False)]
            far = [own[n][1] for n in moment_names(sx, sy, rows_x, True)]
            if sy == 0:
                tiles = near + pack(far, 7, 2)
            elif sy == 1:
                tiles = pack([jnp.where(last_row, a, b) for a, b in zip(near, far)], 7, 2)
            else:
                tiles = pack(far, 7, 1) + pack(near, 0, 2)
            for k, tile in enumerate(tiles):
                put(step, 1, d, k, tile)
            if d == 7:
                launch_far(step, 1)
        launch_near(step, 1)
        for n, sx in enumerate((1, -1)):
            edge = rows_x - 1 if sx == 1 else 0
            for k, q in enumerate(XS[sx]):
                put(step, 2, n, k, moved[q][edge])
        for n, sy in enumerate((1, -1)):
            rows_kept = moved[YS[sy][0]]
            start = 0 if sy == 1 else 7
            for k, q in enumerate(YS[sy][1:], 1):
                rows_kept = jnp.where(sub == (start + k) % 8, roll(moved[q], k, 1), rows_kept)
            for x in range(rows_x):
                put(step, 2, 2 + n, x, rows_kept[x])
        for n, (sx, sy) in enumerate(DIRS[4:]):
            put(step, 2, 4 + n, 0, moved[CORNER[sx, sy]][rows_x - 1 if sx == 1 else 0])
        launch_far(step, 2)
        launch_near(step, 2)
        arrive(step, 1)
        reach = [x for x in range(rows_x + 2)] + [-1]
        near = {(x, c): [] for x in reach for c in range(4)}
        far = {(x, c): [] for x in reach for c in range(4)}
        for name, (a, b) in own.items():
            near[name].append(a)
            far[name].append(b)
        two, edges, one = row_mask(0, 2, depth), row_mask(7, 2, depth), row_mask(7, 1, depth)
        for d, (sx, sy) in enumerate(DIRS):
            names = moment_names(sx, sy, rows_x, False)
            beyond = moment_names(sx, sy, rows_x, True)
            load = lambda k, d=d: got(step, 1, d, k)
            if sy == 0:
                a = [load(k) for k in range(len(names))]
                b = unpack(lambda k: load(len(names) + k), len(beyond), 2)
                b = [jnp.where(edges, t, 0.0) for t in b]
                a, b = dict(zip(names, a)), dict(zip(beyond, b))
            elif sy == 1:
                both_rows = unpack(load, len(names), 2)
                a = dict(zip(names, [jnp.where(first_row, t, 0.0) for t in both_rows]))
                b = dict(zip(names, [jnp.where(last_row, t, 0.0) for t in both_rows]))
            else:
                skip = packed(len(beyond), 1)
                a = [jnp.where(one, t, 0.0) for t in unpack(load, len(beyond), 1)]
                b = unpack(lambda k: load(skip + k), len(names), 2)
                b = [jnp.where(two, t, 0.0) for t in b]
                a, b = dict(zip(beyond, a)), dict(zip(names, b))
            for side, part in ((near, a), (far, b)):
                for (x, c), tile in restore(part, sx, sy, rows_x).items():
                    side[landing(x, sx, rows_x), c].append(tile)
        used = row_mask(7, 3, depth)
        count = len(reach)
        for i, x in enumerate(reach):
            inverse = 1.0 / total_of(near[x, 0])
            for a in range(3):
                wide[a, i] = total_of(near[x, a + 1]) * inverse
        speed = {}
        for x in reach:
            inverse = 1.0 / jnp.where(used, total_of(far[x, 0]), 1.0)
            for a in range(3):
                speed[x, a] = total_of(far[x, a + 1]) * inverse
        for k, y in enumerate(far_y):
            for a in range(3):
                tile = jnp.zeros((8, depth), jnp.float32)
                for x in reach:
                    tile = jnp.where(sub == (x & 7), roll(speed[x, a], x - y, 0), tile)
                wide[a, count + k] = tile
        wide_high, wide_low = split(wide[...].reshape((count + 3) * 24, depth))
        twice = jnp.concatenate([wide_high, wide_high], axis=1)
        pieces = []
        for cut in chunks:
            along = mm(twice, deep[:, cut], NN) + mm(wide_low, deep[0:depth, cut], NN)
            along = along.reshape(3, count + 3, 8, along.shape[1])
            drift = []
            for a in range(3):
                near_sum = total_of([
                    along[a, i] * table_x[x & 7 : (x & 7) + 1, cut] for i, x in enumerate(reach)
                ])
                far_sum = total_of([
                    along[a, count + k] * table_y[y : y + 1, cut] for k, y in enumerate(far_y)
                ])
                total = near_sum * table_y[0:8, cut] + far_sum * table_x[:, cut]
                drift.append(jnp.sum(total, axis=0, keepdims=True))
            pieces.append(jnp.concatenate(drift, axis=0))
        off[...] = now + live * jnp.concatenate(pieces, axis=1)
        return carry

    substep(0, 0, True)
    lax.fori_loop(1, SUBSTEPS, substep, 0)
    finish_pops(SUBSTEPS - 1)

    for m in range(slots):
        offset_out[:, m, :] = off[:, m * padded : (m + 1) * padded]

    pltpu.make_async_remote_copy(
        src_ref=send_buf, dst_ref=recv_buf, send_sem=send_sem.at[0], recv_sem=recv_sem.at[0, 0],
        device_id=peer[0], device_id_type=MESH,
    ).wait_send()


def write_kernel(pops_ref, offset_ref, pops_out, offset_out, sem):
    copies = [
        pltpu.make_async_copy(pops_ref, pops_out, sem.at[0]),
        pltpu.make_async_copy(offset_ref, offset_out, sem.at[1]),
    ]
    for x in copies:
        x.start()
    for x in copies:
        x.wait()


def local(mesh, populations, solid, base_cell, offset, rest, stiffness, occupied, triangles):
    rows_x, rows_y, depth = populations.shape[1:]
    slots, padded = offset.shape[3:]
    assert rows_y == 8 and rows_x == 4 and depth & (depth - 1) == 0
    vertices, planes = slots * padded, rows_x + 3
    S = SUBSTEPS
    f32, bf16 = jnp.float32, jnp.bfloat16
    tile = (8, depth)
    V = lambda shape, dtype=f32: pltpu.VMEM(shape, dtype)
    small = (3, slots, padded)
    i32 = jnp.int32
    scratch = [
        V(solid.shape, i32), V(small, i32), V(small), V(small),
        pltpu.SMEM((slots,), f32), pltpu.SMEM((slots,), i32), V(triangles.shape[::-1], i32),
        V((padded, triangles.shape[0]), bf16),
        V((padded, 2 * padded), bf16), V((3, vertices)),
        V(((planes + 3) * 48 + 32, vertices), bf16), V((2 * depth, vertices), bf16),
        V((3, 24, vertices)), V((3, depth, vertices), bf16),
        V((19, rows_x) + tile), V((3, planes + 3) + tile),
    ]
    tiles = sum(stage_sizes(rows_x, 2)[1], stage_sizes(rows_x, 2)[0])
    scratch += [V((S, tiles) + tile)] * 2
    scratch += [pltpu.SemaphoreType.DMA((1,)), pltpu.SemaphoreType.DMA((S, 3))]
    scratch += [pltpu.SemaphoreType.DMA((8,))]
    vmem = pl.BlockSpec(memory_space=pltpu.VMEM)
    hbm = pl.BlockSpec(memory_space=pltpu.HBM)
    pops, moved = pl.pallas_call(
        functools.partial(body_kernel, mesh.shape["gx"], mesh.shape["gy"]),
        out_shape=(pltpu.VMEM(populations.shape, f32), pltpu.VMEM(small, f32)),
        in_specs=[hbm] * 8,
        out_specs=(vmem, vmem),
        scratch_shapes=scratch,
        compiler_params=pltpu.CompilerParams(
            collective_id=0, has_side_effects=True, vmem_limit_bytes=24 * 1024 * 1024
        ),
    )(*[
        pltpu.with_memory_space_constraint(x, pltpu.HBM)
        for x in (
            populations, solid, base_cell.reshape(small), offset.reshape(small),
            rest.reshape(small), stiffness.reshape(slots), occupied.reshape(slots), triangles.T,
        )
    ])
    pops, moved = pl.pallas_call(
        write_kernel,
        out_shape=(
            jax.ShapeDtypeStruct(populations.shape, f32), jax.ShapeDtypeStruct(small, f32),
        ),
        in_specs=[pl.BlockSpec(memory_space=pl.ANY)] * 2,
        out_specs=(hbm, hbm),
        scratch_shapes=[pltpu.SemaphoreType.DMA((2,))],
        compiler_params=pltpu.CompilerParams(vmem_limit_bytes=1024 * 1024),
    )(pops, moved)
    return pops, moved.reshape(offset.shape)


def solution(mesh):
    in_specs = (
        P(None, "gx", "gy", None),
        P("gx", "gy", None),
        P(None, "gx", "gy", None, None),
        P(None, "gx", "gy", None, None),
        P(None, "gx", "gy", None, None),
        P("gx", "gy", None),
        P("gx", "gy", None),
        P(),
    )
    out_specs = (P(None, "gx", "gy", None), P(None, "gx", "gy", None, None))
    return jax.shard_map(
        functools.partial(local, mesh), mesh=mesh, in_specs=in_specs, out_specs=out_specs,
        check_vma=False,
    )
```

```python
import functools
import math

import jax
import jax.numpy as jnp
from jax import lax
from jax.experimental import pallas as pl
from jax.experimental.pallas import tpu as pltpu
from jax.sharding import PartitionSpec as P

SUBSTEPS = 3
VELOCITIES = [
    (0, 0, 0), (1, 0, 0), (-1, 0, 0), (0, 1, 0), (0, -1, 0), (0, 0, 1), (0, 0, -1),
    (1, 1, 0), (-1, -1, 0), (1, -1, 0), (-1, 1, 0), (1, 0, 1), (-1, 0, -1), (1, 0, -1),
    (-1, 0, 1), (0, 1, 1), (0, -1, -1), (0, 1, -1), (0, -1, 1),
]
OPPOSITE = [0, 2, 1, 4, 3, 6, 5, 8, 7, 10, 9, 12, 11, 14, 13, 16, 15, 18, 17]
LATTICE_WEIGHTS = [1.0 / 3.0] + [1.0 / 18.0] * 6 + [1.0 / 36.0] * 12
RELAX = 0.8
CHUNK = 768
MASKS = (((0, 0.25), (1, 0.25), (2, 0.25), (3, 0.25)), ((1, 1.0), (3, -1.0)), ((2, 1.0), (0, -1.0)))
XS = {s: [q for q in range(19) if VELOCITIES[q][0] == s] for s in (1, -1)}
YS = {s: [q for q in range(19) if VELOCITIES[q][1] == s] for s in (1, -1)}
CORNER = {(v[0], v[1]): q for q, v in enumerate(VELOCITIES) if v[0] and v[1]}
DIRS = [(1, 0), (-1, 0), (0, 1), (0, -1), (1, 1), (1, -1), (-1, 1), (-1, -1)]
MESH = pl.DeviceIdType.MESH
NT = (((1,), (1,)), ((), ()))
NN = (((1,), (0,)), ((), ()))


def mm(a, b, dims):
    return lax.dot_general(a, b, dims, preferred_element_type=jnp.float32)


def split(value):
    high = value.astype(jnp.bfloat16)
    low = (value - high.astype(jnp.float32)).astype(jnp.bfloat16)
    return high, low


def quarter_sine(t):
    t = t - 4.0 * jnp.floor(t * 0.25 + 0.5)
    t = jnp.maximum(jnp.minimum(t, 2.0 - t), -2.0 - t)
    x = t * (math.pi / 2.0)
    u = x * x
    p = 1.0 / 6227020800.0
    for c in (-1.0 / 39916800.0, 1.0 / 362880.0, -1.0 / 5040.0, 1.0 / 120.0, -1.0 / 6.0, 1.0):
        p = p * u + c
    return x * p


def distance(rows, base):
    cells = lax.broadcasted_iota(jnp.int32, (rows, base.shape[1]), 0)
    return (cells - base + 1) & (rows - 1)


def moments(pops):
    density = functools.reduce(lambda a, b: a + b, pops)
    momentum = []
    for a in range(3):
        plus = [pops[q] for q in range(19) if VELOCITIES[q][a] == 1]
        minus = [pops[q] for q in range(19) if VELOCITIES[q][a] == -1]
        momentum.append(
            functools.reduce(lambda a, b: a + b, plus)
            - functools.reduce(lambda a, b: a + b, minus)
        )
    return density, momentum


def settle(pops, walled):
    density, momentum = moments(pops)
    kept = 1.0 - 1.0 / RELAX
    still = [jnp.where(walled, pops[OPPOSITE[q]], kept * pops[q]) for q in range(19)]
    return density, momentum, still


def collide(density, momentum, still, force, walled):
    inverse = 1.0 / density
    rate, keep = 1.0 / RELAX, 1.0 - 0.5 / RELAX
    n = [momentum[a] + 0.5 * force[a] for a in range(3)]
    u = [jnp.where(walled, 0.0, n[a] * inverse) for a in range(3)]
    squared = u[0] * n[0] + u[1] * n[1] + u[2] * n[2]
    working = u[0] * force[0] + u[1] * force[1] + u[2] * force[2]
    even = rate * density - (1.5 * rate) * squared - (3.0 * keep) * working
    w = LATTICE_WEIGHTS[1]
    odd = [(3.0 * rate * w) * n[a] + (3.0 * keep * w) * force[a] for a in range(3)]
    twice = [(4.5 * rate * w) * n[a] + (9.0 * keep * w) * force[a] for a in range(3)]
    even = jnp.where(walled, 0.0, even)
    odd = [jnp.where(walled, 0.0, x) for x in odd]
    axis_even, half_even = w * even, (0.5 * w) * even
    half_odd, half_twice = [0.5 * x for x in odd], [0.5 * x for x in twice]

    def dot(vector, values):
        terms = [(vector[a], values[a]) for a in range(3) if vector[a]]
        out = terms[0][1] if terms[0][0] == 1 else -terms[0][1]
        for sign, value in terms[1:]:
            out = out + value if sign == 1 else out - value
        return out

    fresh = {0: LATTICE_WEIGHTS[0] * even}
    for q in range(1, 19, 2):
        vector = VELOCITIES[q]
        diagonal = sum(abs(v) for v in vector) == 2
        push = dot(vector, half_odd if diagonal else odd)
        mid = (half_even if diagonal else axis_even) + dot(vector, u) * dot(
            vector, half_twice if diagonal else twice
        )
        fresh[q], fresh[OPPOSITE[q]] = mid + push, mid - push
    return [still[q] + fresh[q] for q in range(19)]


def roll(x, shift, axis):
    size = x.shape[axis]
    shift = shift % size
    return x if shift == 0 else pltpu.roll(x, shift, axis)


def row_mask(start, rows, depth):
    sub = lax.broadcasted_iota(jnp.int32, (8, depth), 0)
    return ((sub - start) & 7) < rows


def pack(tiles, start, rows):
    per, out = 8 // rows, []
    for g in range(0, len(tiles), per):
        acc = tiles[g]
        for k, tile in enumerate(tiles[g + 1 : g + per], 1):
            mask = row_mask(start + k * rows, rows, tile.shape[1])
            acc = jnp.where(mask, roll(tile, k * rows, 0), acc)
        out.append(acc)
    return out


def unpack(load, count, rows):
    per = 8 // rows
    return [roll(load(k // per), -(k % per) * rows, 0) for k in range(count)]


def packed(count, rows):
    return -(-count // (8 // rows))


def force_planes(sx, rows_x):
    return {1: [rows_x, rows_x + 1], -1: [-1], 0: list(range(rows_x))}[sx]


def moment_planes(sx, rows_x):
    return {1: [rows_x - 1, rows_x], -1: [-1, 0, 1], 0: list(range(-1, rows_x + 1))}[sx]


def landing(x, sx, rows_x):
    return x - sx * rows_x


def force_size(sx, sy, rows_x):
    n = 3 * len(force_planes(sx, rows_x))
    return n if sy == 0 else -(-n * (2 if sy == 1 else 1) // 8)


def moment_names(sx, sy, rows_x, beyond):
    names = []
    for x in moment_planes(sx, rows_x):
        ring = x in (-1, rows_x)
        if beyond and sy == -1:
            names += [(x, c) for c in ((0,) if ring else (0, 1, 3))]
        else:
            names += [(x, c) for c in ((0, 2, 3) if ring else (0, 1, 2, 3))]
    return names


def restore(part, sx, sy, rows_x):
    for x in moment_planes(sx, rows_x):
        ring = {-1: -1.0, rows_x: 1.0}.get(x)
        if (x, 1) not in part:
            part[x, 1] = ring * part[x, 0]
        if (x, 2) not in part:
            part[x, 2] = float(sy) * part[x, 0]
    return part


def moment_size(sx, sy, rows_x):
    near, far = (len(moment_names(sx, sy, rows_x, k)) for k in (False, True))
    return {0: near + packed(far, 2), 1: packed(near, 2), -1: packed(far, 1) + packed(near, 2)}[sy]


def halved(sums):
    return total_of([0.5 * x for x in sums if x is not None])


def stage_sizes(rows_x, stage):
    force = [force_size(*d, rows_x) for d in DIRS]
    moment = [moment_size(*d, rows_x) for d in DIRS]
    pops = [len(XS[1])] * 2 + [rows_x] * 2 + [1] * 4
    sizes = (force, moment, pops)
    return sum(sum(x) for x in sizes[:stage]), sizes[stage]


def total_of(parts):
    return functools.reduce(lambda a, b: a + b, parts)


def body_kernel(
    peers_x, peers_y,
    pops_hbm, solid_hbm, base_hbm, offset_hbm, rest_hbm, stiff_hbm, occ_hbm, tri_hbm,
    pops_out, offset_out,
    solid_ref, base_ref, offset_ref, rest_ref, stiff_ref, occ_ref, tri_ref,
    incidence, lap, off, spread, deep, masks, masks_z, moved_ref, wide,
    send_buf, recv_buf, send_sem, recv_sem, load_sem,
):
    rows_x = pops_out.shape[1]
    depth = pops_out.shape[3]
    slots, padded = base_ref.shape[1], base_ref.shape[2]
    vertices = slots * padded
    chunks = [slice(k, min(k + CHUNK, vertices)) for k in range(0, vertices, CHUNK)]
    ix, iy = lax.axis_index("gx"), lax.axis_index("gy")
    peer = [((ix + sx + peers_x) % peers_x, (iy + sy + peers_y) % peers_y) for sx, sy in DIRS]

    loads = [
        pltpu.make_async_copy(src, dst, load_sem.at[k])
        for k, (src, dst) in enumerate((
            (tri_hbm, tri_ref), (offset_hbm, offset_ref), (rest_hbm, rest_ref),
            (base_hbm, base_ref), (stiff_hbm, stiff_ref), (occ_hbm, occ_ref),
            (solid_hbm, solid_ref), (pops_hbm, pops_out),
        ))
    ]
    for x in loads:
        x.start()
    barrier = pltpu.get_barrier_semaphore()
    for p in peer:
        pl.semaphore_signal(barrier, inc=1, device_id=p, device_id_type=MESH)

    for x in loads[:6]:
        x.wait()
    faces = tri_ref.shape[1]
    parts = [slice(k, min(k + 256, faces)) for k in range(0, faces, 256)]

    def build_laplacian():
        sums = [None, None]
        for c, cut in enumerate(parts):
            part = mm(incidence[:, cut], incidence[:, cut], NT)
            sums[c % 2] = part if sums[c % 2] is None else sums[c % 2] + part
        pairs = halved(sums) * 2.0
        same = lax.broadcasted_iota(jnp.int32, pairs.shape, 0) == lax.broadcasted_iota(
            jnp.int32, pairs.shape, 1
        )
        lap_high, lap_low = split(jnp.where(same, -2.0 * pairs, pairs))
        lap[:, 0:padded] = lap_high
        lap[:, padded:] = -lap_low

    def flat(ref):
        return jnp.concatenate([ref[:, m, :] for m in range(slots)], axis=1)

    base = flat(base_ref)
    base_x = base[0:1] - ix * rows_x
    base_y = base[1:2] - iy * pops_out.shape[2]
    base_z = base[2:3]
    live = jnp.concatenate(
        [jnp.full((1, padded), occ_ref[m].astype(jnp.float32)) for m in range(slots)], axis=1
    )
    scale = live * jnp.concatenate(
        [jnp.full((1, padded), stiff_ref[m]) for m in range(slots)], axis=1
    )
    lane = lax.broadcasted_iota(jnp.int32, scale.shape, 1)
    scale = jnp.where((lane // CHUNK) % 2 == 1, -scale, scale)
    off[...] = flat(offset_ref)
    sub = lax.broadcasted_iota(jnp.int32, (8, depth), 0)
    distances = ((8, base_x, 0), (16, base_y, 8), (depth, base_z, 24))

    short = lambda x: jnp.broadcast_to(x, (depth, vertices)).astype(jnp.int16)
    cells = lax.broadcasted_iota(jnp.int32, (depth, vertices), 0) + 1
    d = (short(cells) - short(base_z)) & short(jnp.int32(depth - 1))
    unit = jnp.ones(d.shape, jnp.bfloat16)
    for k, pairs in enumerate(MASKS):
        value = 0.0 * unit
        for j, weight in pairs:
            value = jnp.where(d == short(jnp.int32(j)), weight * unit, value)
        masks_z[k] = value
    for rows, base_row, start in distances[:2]:
        d = distance(rows, base_row)
        fits = [
            jnp.where(d < 4, 0.25, 0.0),
            jnp.where(d == 1, 1.0, jnp.where(d == 3, -1.0, 0.0)),
            jnp.where(d == 2, 1.0, jnp.where(d == 0, -1.0, 0.0)),
        ]
        for k in range(3):
            masks[k, start : start + rows, :] = fits[k]

    def place(stage, d):
        start = stage_sizes(rows_x, stage)[0]
        sizes = stage_sizes(rows_x, stage)[1]
        return start + sum(sizes[:d]), sizes[d]

    def copy(step, stage, start, size, device):
        part = pl.ds(start, size)
        return pltpu.make_async_remote_copy(
            src_ref=send_buf.at[step, part], dst_ref=recv_buf.at[step, part],
            send_sem=send_sem.at[0], recv_sem=recv_sem.at[step, stage],
            device_id=device, device_id_type=MESH,
        )

    def whole(step, stage):
        start, sizes = stage_sizes(rows_x, stage)
        return copy(step, stage, start, sum(sizes), peer[0])

    def put(step, stage, d, k, tile):
        send_buf[step, place(stage, d)[0] + k] = tile

    def got(step, stage, d, k):
        return recv_buf[step, place(stage, d)[0] + k]

    def launch_far(step, stage):
        sends = {DIRS[d]: copy(step, stage, *place(stage, d), peer[d]) for d in range(2, 8)}
        for side in (0, 1):
            for part in (0, 1):
                near = 1 if side == 0 else -1
                far = 1 if part == 1 else -1
                turn = (0, -near, near) if side == 0 else (-near, near, 0)
                order = [(x, y) for y in (far, -far) for x in turn]

                @pl.when((ix % 2 == side) & (iy % 2 == part))
                def _(order=order):
                    for name in order:
                        sends[name].start()

    def launch_near(step, stage):
        for d in (1, 0):
            copy(step, stage, *place(stage, d), peer[d]).start()

    def arrive(step, stage):
        whole(step, stage).wait_recv()

    def finish_pops(step):
        arrive(step, 2)
        from_y = {
            sy: jnp.stack([got(step, 2, d, x) for x in range(rows_x)]) for d, sy in ((2, 1), (3, -1))
        }
        for q in range(19):
            sx, sy, _ = VELOCITIES[q]
            value = moved_ref[q]
            edge_row = sub == (0 if sy == 1 else 7)
            if sy:
                value = jnp.where(edge_row, roll(from_y[sy], -YS[sy].index(q), 1), value)
            if sx:
                side = got(step, 2, 0 if sx == 1 else 1, XS[sx].index(q))
                if sy:
                    side = jnp.where(edge_row, got(step, 2, DIRS.index((sx, sy)), 0), side)
                if sx == 1:
                    value = jnp.concatenate([side[None], value[:-1]], axis=0)
                else:
                    value = jnp.concatenate([value[1:], side[None]], axis=0)
            pops_out[q] = value

    def stacked(value):
        high = value.astype(jnp.bfloat16).astype(jnp.float32)
        return jnp.concatenate([high, value - high], axis=0).astype(jnp.bfloat16)

    def substep(step, carry, first=False):
        now = off[...]
        waves = quarter_sine(jnp.concatenate([now, now + 1.0], axis=0)) * 0.25
        table_x, table_y = [
            masks[0, start : start + rows, :]
            + waves[3 + k : 4 + k] * masks[1, start : start + rows, :]
            + waves[k : k + 1] * masks[2, start : start + rows, :]
            for k, (rows, _, start) in enumerate(distances[:2])
        ]
        coarse = jnp.floor(waves * 512.0 + 0.5) * (1.0 / 512.0)
        fine = waves - coarse
        sine, cosine, sine_low, cosine_low = [
            jnp.broadcast_to(x, (depth, vertices)).astype(jnp.bfloat16)
            for x in (coarse[2:3], coarse[5:6], fine[2:3], fine[5:6])
        ]
        deep[0:depth, :] = masks_z[0] + cosine * masks_z[1] + sine * masks_z[2]
        deep[depth:, :] = cosine_low * masks_z[1] + sine_low * masks_z[2]
        strain = now - flat(rest_ref)
        six = jnp.concatenate(
            [strain[:, m * padded : (m + 1) * padded] for m in range(slots)], axis=0
        )
        if first:
            sums, pair = [None, None], stacked(six)
            for c, cut in enumerate(parts):
                shape = (padded, cut.stop - cut.start)
                ids = lax.broadcasted_iota(jnp.int32, shape, 0).astype(jnp.int16)
                hit = None
                for k in range(3):
                    corner = jnp.broadcast_to(tri_ref[k : k + 1, cut], shape).astype(jnp.int16)
                    hit = ids == corner if hit is None else hit | (ids == corner)
                one = jnp.ones(shape, jnp.bfloat16)
                incidence[:, cut] = jnp.where(hit, one, jnp.zeros(shape, jnp.bfloat16))
                summed = mm(pair, incidence[:, cut], NN)
                summed = summed[0 : 3 * slots] + summed[3 * slots :]
                ones = jnp.ones((1, summed.shape[1]), jnp.bfloat16)
                part = mm(
                    jnp.concatenate([stacked(summed), ones], axis=0), incidence[:, cut], NT
                )
                sums[c % 2] = part if sums[c % 2] is None else sums[c % 2] + part
            pulled = halved(sums) * 2.0
            count = pulled[6 * slots :]
            pulled = pulled[0 : 3 * slots] + pulled[3 * slots : 6 * slots]
            pulled = pulled - 3.0 * count * six
        else:
            both = stacked(six)
            pulled = mm(both, lap[:, 0:padded], NN) - mm(both, lap[:, padded:], NN)
            pulled = pulled[0 : 3 * slots] + pulled[3 * slots :]
        force_v = scale * jnp.concatenate(
            [pulled[3 * m : 3 * m + 3] for m in range(slots)], axis=1
        )
        pulled_x = [force_v[a : a + 1] * table_x for a in range(3)]
        tiles_of = {}

        def spread_tiles(names, start):
            half, sums = 16 * -(-len(names) // 2), [None, None]
            for c, cut in enumerate(chunks):
                for n in range(0, len(names), 2):
                    blocks = [
                        pulled_x[a][:, cut] * table_y[y : y + 1, cut] if x is None
                        else pulled_x[a][x & 7 : (x & 7) + 1, cut] * table_y[0:8, cut]
                        for x, a, y in names[n : n + 2]
                    ]
                    if len(blocks) == 1:
                        blocks = blocks * 2
                    high, low = split(jnp.concatenate(blocks, axis=0))
                    row = start + 8 * n
                    spread[row : row + 16, cut] = high
                    spread[row + half : row + half + 16, cut] = low
                part = mm(spread[start : start + 2 * half, cut], deep[:, cut], NT)
                sums[c % 2] = part if sums[c % 2] is None else sums[c % 2] + part
            total = sums[0] - sums[1]
            total = total[:half, :depth] + total[:half, depth:] + total[half:, :depth]
            for n, name in enumerate(names):
                tiles_of[name] = total[8 * n : 8 * n + 8]

        far_y = (8, 9, 15)
        outer = [(None, a, y) for y in far_y for a in range(3)]
        outer += [(x, a, 0) for x in (rows_x, rows_x + 1, -1) for a in range(3)]
        spread_tiles(outer, 0)
        def put_force(d):
            sx, sy = DIRS[d]
            across = force_planes(sx, rows_x)
            if sy == 0:
                tiles = [tiles_of[x, a, 0] for x in across for a in range(3)]
            else:
                tiles = [
                    tiles_of[None, a, y] for y in ((8, 9) if sy == 1 else (15,)) for a in range(3)
                ]
                tiles = pack(tiles, across[0] & 7, len(across))
            for k, tile in enumerate(tiles):
                put(step, 0, d, k, tile)

        for d in range(8):
            put_force(d)
        if first:
            pl.semaphore_wait(barrier, len(peer))
        launch_far(step, 0)
        launch_near(step, 0)
        inner = [(x, a, 0) for x in range(rows_x) for a in range(3)]
        spread_tiles(inner, 16 * len(outer))
        if first:
            build_laplacian()
            loads[6].wait()
            loads[7].wait()
        else:
            finish_pops(step - 1)

        walled = solid_ref[...] != 0
        density, momentum, still = settle([pops_out[q] for q in range(19)], walled)
        for q in range(19):
            pops_out[q] = still[q]
        arrive(step, 0)
        force = [[tiles_of[x, a, 0] for x in range(rows_x)] for a in range(3)]
        edge = {(y, a): None for y in (0, 1, 7) for a in range(3)}
        for d, (sx, sy) in enumerate(DIRS):
            load = lambda k, d=d: got(step, 0, d, k)
            planes_in = force_planes(sx, rows_x)
            if sy == 0:
                for k, x in enumerate(planes_in):
                    for a in range(3):
                        here = force[a][landing(x, sx, rows_x)]
                        force[a][landing(x, sx, rows_x)] = here + load(3 * k + a)
                continue
            names = [(y, a) for y in ((0, 1) if sy == 1 else (7,)) for a in range(3)]
            rows, per = len(planes_in), 8 // len(planes_in)
            sent, land = planes_in[0] & 7, landing(planes_in[0], sx, rows_x)
            mask = row_mask(land, rows, depth)
            for k, name in enumerate(names):
                tile = roll(load(k // per), land - sent - (k % per) * rows, 0)
                tile = jnp.where(mask, tile, 0.0)
                edge[name] = tile if edge[name] is None else edge[name] + tile
        for a in range(3):
            for x in range(rows_x):
                tile = jnp.where(sub == 0, roll(edge[0, a], -x, 0), 0.0)
                for y in (1, 7):
                    tile = jnp.where(sub == y, roll(edge[y, a], y - x, 0), tile)
                force[a][x] = force[a][x] + tile
        force = [jnp.stack(force[a]) for a in range(3)]

        relaxed = collide(
            density, momentum, [pops_out[q] for q in range(19)], force, walled
        )
        moved = [
            roll(roll(relaxed[q], VELOCITIES[q][2], 2), VELOCITIES[q][1], 1) for q in range(19)
        ]
        for q in range(19):
            moved_ref[q] = moved[q]
        nothing = jnp.zeros((1, 8, depth), jnp.float32)
        rho, mz = {}, {}
        for cx in (-1, 0, 1):
            for cy in (-1, 0, 1):
                members = [q for q in range(19) if VELOCITIES[q][:2] == (cx, cy)]
                pad = lambda v: jnp.concatenate(
                    [nothing] * (1 + cx) + [v] + [nothing] * (1 - cx), axis=0
                )
                rho[cx, cy] = pad(total_of([moved[q] for q in members]))
                up = [moved[q] for q in members if VELOCITIES[q][2] == 1]
                down = [moved[q] for q in members if VELOCITIES[q][2] == -1]
                if up:
                    mz[cx, cy] = pad(total_of(up) - total_of(down))
        first_row, last_row = sub == 0, sub == 7
        own = {}
        zero = jnp.zeros((rows_x + 2, 8, depth), jnp.float32)
        fields = []
        for cy in (0, 1, -1):
            dens = rho[-1, cy] + rho[0, cy] + rho[1, cy]
            deep_m = [mz[cx, cy] for cx in (-1, 0, 1) if (cx, cy) in mz]
            fields.append((
                dens, rho[1, cy] - rho[-1, cy], zero if cy == 0 else cy * dens, total_of(deep_m)
            ))
        for c in range(4):
            mid, up, down = (fields[g][c] for g in range(3))
            near = mid + jnp.where(first_row, 0.0, up) + jnp.where(last_row, 0.0, down)
            if c:
                half = 0.5 * force[c - 1]
                near = near + jnp.concatenate([nothing, half, nothing], axis=0)
            far = jnp.where(first_row, up, jnp.where(last_row, down, 0.0))
            for x in range(-1, rows_x + 1):
                own[x, c] = (near[x + 1], far[x + 1])
        for d in (2, 3, 4, 5, 6, 7, 0, 1):
            sx, sy = DIRS[d]
            near = [own[n][0] for n in moment_names(sx, sy, rows_x, False)]
            far = [own[n][1] for n in moment_names(sx, sy, rows_x, True)]
            if sy == 0:
                tiles = near + pack(far, 7, 2)
            elif sy == 1:
                tiles = pack([jnp.where(last_row, a, b) for a, b in zip(near, far)], 7, 2)
            else:
                tiles = pack(far, 7, 1) + pack(near, 0, 2)
            for k, tile in enumerate(tiles):
                put(step, 1, d, k, tile)
            if d == 7:
                launch_far(step, 1)
        launch_near(step, 1)
        for n, sx in enumerate((1, -1)):
            edge = rows_x - 1 if sx == 1 else 0
            for k, q in enumerate(XS[sx]):
                put(step, 2, n, k, moved[q][edge])
        for n, sy in enumerate((1, -1)):
            rows_kept = moved[YS[sy][0]]
            start = 0 if sy == 1 else 7
            for k, q in enumerate(YS[sy][1:], 1):
                rows_kept = jnp.where(sub == (start + k) % 8, roll(moved[q], k, 1), rows_kept)
            for x in range(rows_x):
                put(step, 2, 2 + n, x, rows_kept[x])
        for n, (sx, sy) in enumerate(DIRS[4:]):
            put(step, 2, 4 + n, 0, moved[CORNER[sx, sy]][rows_x - 1 if sx == 1 else 0])
        launch_far(step, 2)
        launch_near(step, 2)
        arrive(step, 1)
        reach = [x for x in range(rows_x + 2)] + [-1]
        near = {(x, c): [] for x in reach for c in range(4)}
        far = {(x, c): [] for x in reach for c in range(4)}
        for name, (a, b) in own.items():
            near[name].append(a)
            far[name].append(b)
        two, edges, one = row_mask(0, 2, depth), row_mask(7, 2, depth), row_mask(7, 1, depth)
        for d, (sx, sy) in enumerate(DIRS):
            names = moment_names(sx, sy, rows_x, False)
            beyond = moment_names(sx, sy, rows_x, True)
            load = lambda k, d=d: got(step, 1, d, k)
            if sy == 0:
                a = [load(k) for k in range(len(names))]
                b = unpack(lambda k: load(len(names) + k), len(beyond), 2)
                b = [jnp.where(edges, t, 0.0) for t in b]
                a, b = dict(zip(names, a)), dict(zip(beyond, b))
            elif sy == 1:
                both_rows = unpack(load, len(names), 2)
                a = dict(zip(names, [jnp.where(first_row, t, 0.0) for t in both_rows]))
                b = dict(zip(names, [jnp.where(last_row, t, 0.0) for t in both_rows]))
            else:
                skip = packed(len(beyond), 1)
                a = [jnp.where(one, t, 0.0) for t in unpack(load, len(beyond), 1)]
                b = unpack(lambda k: load(skip + k), len(names), 2)
                b = [jnp.where(two, t, 0.0) for t in b]
                a, b = dict(zip(beyond, a)), dict(zip(names, b))
            for side, part in ((near, a), (far, b)):
                for (x, c), tile in restore(part, sx, sy, rows_x).items():
                    side[landing(x, sx, rows_x), c].append(tile)
        used = row_mask(7, 3, depth)
        count = len(reach)
        for i, x in enumerate(reach):
            inverse = 1.0 / total_of(near[x, 0])
            for a in range(3):
                wide[a, i] = total_of(near[x, a + 1]) * inverse
        speed = {}
        for x in reach:
            inverse = 1.0 / jnp.where(used, total_of(far[x, 0]), 1.0)
            for a in range(3):
                speed[x, a] = total_of(far[x, a + 1]) * inverse
        for k, y in enumerate(far_y):
            for a in range(3):
                tile = jnp.zeros((8, depth), jnp.float32)
                for x in reach:
                    tile = jnp.where(sub == (x & 7), roll(speed[x, a], x - y, 0), tile)
                wide[a, count + k] = tile
        wide_high, wide_low = split(wide[...].reshape((count + 3) * 24, depth))
        twice = jnp.concatenate([wide_high, wide_high], axis=1)
        pieces = []
        for cut in chunks:
            along = mm(twice, deep[:, cut], NN) + mm(wide_low, deep[0:depth, cut], NN)
            along = along.reshape(3, count + 3, 8, along.shape[1])
            drift = []
            for a in range(3):
                near_sum = total_of([
                    along[a, i] * table_x[x & 7 : (x & 7) + 1, cut] for i, x in enumerate(reach)
                ])
                far_sum = total_of([
                    along[a, count + k] * table_y[y : y + 1, cut] for k, y in enumerate(far_y)
                ])
                total = near_sum * table_y[0:8, cut] + far_sum * table_x[:, cut]
                drift.append(jnp.sum(total, axis=0, keepdims=True))
            pieces.append(jnp.concatenate(drift, axis=0))
        off[...] = now + live * jnp.concatenate(pieces, axis=1)
        return carry

    for step in range(SUBSTEPS):
        substep(step, 0, step == 0)
    finish_pops(SUBSTEPS - 1)

    for m in range(slots):
        offset_out[:, m, :] = off[:, m * padded : (m + 1) * padded]

    pltpu.make_async_remote_copy(
        src_ref=send_buf, dst_ref=recv_buf, send_sem=send_sem.at[0], recv_sem=recv_sem.at[0, 0],
        device_id=peer[0], device_id_type=MESH,
    ).wait_send()


def write_kernel(pops_ref, offset_ref, pops_out, offset_out, sem):
    copies = [
        pltpu.make_async_copy(pops_ref, pops_out, sem.at[0]),
        pltpu.make_async_copy(offset_ref, offset_out, sem.at[1]),
    ]
    for x in copies:
        x.start()
    for x in copies:
        x.wait()


def local(mesh, populations, solid, base_cell, offset, rest, stiffness, occupied, triangles):
    rows_x, rows_y, depth = populations.shape[1:]
    slots, padded = offset.shape[3:]
    assert rows_y == 8 and rows_x == 4 and depth & (depth - 1) == 0
    vertices, planes = slots * padded, rows_x + 3
    S = SUBSTEPS
    f32, bf16 = jnp.float32, jnp.bfloat16
    tile = (8, depth)
    V = lambda shape, dtype=f32: pltpu.VMEM(shape, dtype)
    small = (3, slots, padded)
    i32 = jnp.int32
    scratch = [
        V(solid.shape, i32), V(small, i32), V(small), V(small),
        pltpu.SMEM((slots,), f32), pltpu.SMEM((slots,), i32), V(triangles.shape[::-1], i32),
        V((padded, triangles.shape[0]), bf16),
        V((padded, 2 * padded), bf16), V((3, vertices)),
        V(((planes + 3) * 48 + 32, vertices), bf16), V((2 * depth, vertices), bf16),
        V((3, 24, vertices)), V((3, depth, vertices), bf16),
        V((19, rows_x) + tile), V((3, planes + 3) + tile),
    ]
    tiles = sum(stage_sizes(rows_x, 2)[1], stage_sizes(rows_x, 2)[0])
    scratch += [V((S, tiles) + tile)] * 2
    scratch += [pltpu.SemaphoreType.DMA((1,)), pltpu.SemaphoreType.DMA((S, 3))]
    scratch += [pltpu.SemaphoreType.DMA((8,))]
    vmem = pl.BlockSpec(memory_space=pltpu.VMEM)
    hbm = pl.BlockSpec(memory_space=pltpu.HBM)
    pops, moved = pl.pallas_call(
        functools.partial(body_kernel, mesh.shape["gx"], mesh.shape["gy"]),
        out_shape=(pltpu.VMEM(populations.shape, f32), pltpu.VMEM(small, f32)),
        in_specs=[hbm] * 8,
        out_specs=(vmem, vmem),
        scratch_shapes=scratch,
        compiler_params=pltpu.CompilerParams(
            collective_id=0, has_side_effects=True, vmem_limit_bytes=24 * 1024 * 1024,
        ),
    )(*[
        pltpu.with_memory_space_constraint(x, pltpu.HBM)
        for x in (
            populations, solid, base_cell.reshape(small), offset.reshape(small),
            rest.reshape(small), stiffness.reshape(slots), occupied.reshape(slots), triangles.T,
        )
    ])
    pops, moved = pl.pallas_call(
        write_kernel,
        out_shape=(
            jax.ShapeDtypeStruct(populations.shape, f32), jax.ShapeDtypeStruct(small, f32),
        ),
        in_specs=[pl.BlockSpec(memory_space=pl.ANY)] * 2,
        out_specs=(hbm, hbm),
        scratch_shapes=[pltpu.SemaphoreType.DMA((2,))],
        compiler_params=pltpu.CompilerParams(vmem_limit_bytes=1024 * 1024),
    )(pops, moved)
    return pops, moved.reshape(offset.shape)


def solution(mesh):
    in_specs = (
        P(None, "gx", "gy", None),
        P("gx", "gy", None),
        P(None, "gx", "gy", None, None),
        P(None, "gx", "gy", None, None),
        P(None, "gx", "gy", None, None),
        P("gx", "gy", None),
        P("gx", "gy", None),
        P(),
    )
    out_specs = (P(None, "gx", "gy", None), P(None, "gx", "gy", None, None))
    return jax.shard_map(
        functools.partial(local, mesh), mesh=mesh, in_specs=in_specs, out_specs=out_specs,
        check_vma=False,
    )
```
